32 devices in a mesh: dp: 2 (over x), tp: 16 (over z, y, core).
Axes of the slice: x: 2, y: 2, z: 4, core: 2. Of those that a mesh axis runs over, the one named last changes fastest.
Arguments:
- token_ids: int32 [16, 1536], P('dp'), parts along dimension 0
- word_table: bfloat16 [51200, 1536], P('tp')
- pos_table: bfloat16 [1536, 1536], replicated
- ln_gain: float32 [1536], replicated
- ln_bias: float32 [1536], replicated
- w_qkv: bfloat16 [1536, 3, 16, 96], P(None, None, 'tp')
- b_qkv: float32 [3, 16, 96], P(None, 'tp')
- w_out: bfloat16 [16, 96, 1536], P('tp')
- b_out: float32 [1536], replicated
Outputs:
- output 1: bfloat16 [16, 1536, 1536], P('dp', 'tp'), parts along dimension 0
- output 2: bfloat16 [16, 1536, 1536], P('dp', 'tp'), parts along dimension 0
There are 2 independent parts. The reference program is written for one: setup_inputs(seed, part) draws one part's arguments, and reference() takes and returns one part's arrays. A program takes and returns all parts, laid end to end along the dimension named above; an argument that names none is the same for every part.
All inputs are finite; a program needn't handle non-finite values.
Results may differ from the reference program's by a relative error of at most 0.00805794.
Values are sent between devices in bfloat16 or wider.
A program may use at most 1 GiB of HBM per device.

```python
import math
import jax
import jax.numpy as jnp
from jax import lax

VOCAB_SIZE = 51200
MODEL_DIM = 1536
NUM_HEADS = 16
HEAD_DIM = 96
SEQ_LEN = 1536
GROUP_BATCH = 8
OCTAVES = math.ceil(math.log2(VOCAB_SIZE))
LN_EPS = 1e-5


def draw_token_ids(key):
    key_octave, key_rank, key_order = jax.random.split(key, 3)
    id_shape = (GROUP_BATCH, SEQ_LEN)
    octave = jax.random.randint(key_octave, id_shape, 0, OCTAVES + 1)
    rank_span = jnp.minimum(jnp.left_shift(jnp.ones(id_shape, jnp.int32), octave), VOCAB_SIZE)
    rank = jax.random.randint(key_rank, id_shape, 0, rank_span)
    vocab_order = jax.random.permutation(key_order, VOCAB_SIZE)
    return jnp.take(vocab_order, rank).astype(jnp.int32)


def setup_inputs(seed: int = 0, part: int = 0) -> dict:
    base_key = jax.random.key(seed)
    part_key = jax.random.fold_in(base_key, part)
    keys = jax.random.split(base_key, 8)
    token_ids = draw_token_ids(part_key)
    word_table = (0.8 * jax.random.normal(keys[0], (VOCAB_SIZE, MODEL_DIM), jnp.float32)).astype(jnp.bfloat16)
    pos_table = (0.6 * jax.random.normal(keys[1], (SEQ_LEN, MODEL_DIM), jnp.float32)).astype(jnp.bfloat16)
    ln_gain = 1.0 + 0.2 * jax.random.normal(keys[2], (MODEL_DIM,), jnp.float32)
    ln_bias = 0.2 * jax.random.normal(keys[3], (MODEL_DIM,), jnp.float32)
    qkv_scale = jnp.array([3.0 ** 0.5, 3.0 ** 0.5, 1.0], jnp.float32) * MODEL_DIM ** -0.5
    w_qkv = (jax.random.normal(keys[4], (MODEL_DIM, 3, NUM_HEADS, HEAD_DIM), jnp.float32) * qkv_scale[None, :, None, None]).astype(jnp.bfloat16)
    b_qkv = 0.3 * jax.random.normal(keys[5], (3, NUM_HEADS, HEAD_DIM), jnp.float32)
    w_out = (jax.random.normal(keys[6], (NUM_HEADS, HEAD_DIM, MODEL_DIM), jnp.float32) * (NUM_HEADS * HEAD_DIM) ** -0.5).astype(jnp.bfloat16)
    b_out = 0.3 * jax.random.normal(keys[7], (MODEL_DIM,), jnp.float32)
    return {"token_ids": token_ids, "word_table": word_table, "pos_table": pos_table, "ln_gain": ln_gain, "ln_bias": ln_bias, "w_qkv": w_qkv, "b_qkv": b_qkv, "w_out": w_out, "b_out": b_out}


def layer_norm(values, gain, bias):
    feat_mean = jnp.mean(values, axis=-1, keepdims=True)
    centered = values - feat_mean
    feat_variance = jnp.mean(centered * centered, axis=-1, keepdims=True)
    return centered * lax.rsqrt(feat_variance + LN_EPS) * gain + bias


def reference(token_ids, word_table, pos_table, ln_gain, ln_bias, w_qkv, b_qkv, w_out, b_out):
    table_rows = jnp.take(word_table, token_ids, axis=0).astype(jnp.float32)
    embed = (table_rows + pos_table.astype(jnp.float32)[None]).astype(jnp.bfloat16)
    normed = layer_norm(embed.astype(jnp.float32), ln_gain, ln_bias).astype(jnp.bfloat16)
    inner_width = NUM_HEADS * HEAD_DIM
    projected = jnp.dot(normed.reshape(GROUP_BATCH * SEQ_LEN, MODEL_DIM), w_qkv.reshape(MODEL_DIM, 3 * inner_width), preferred_element_type=jnp.float32)
    projected = (projected.reshape(GROUP_BATCH, SEQ_LEN, 3, NUM_HEADS, HEAD_DIM) + b_qkv).astype(jnp.bfloat16)
    heads_first = jnp.transpose(projected, (2, 0, 3, 1, 4)).reshape(3, GROUP_BATCH * NUM_HEADS, SEQ_LEN, HEAD_DIM)
    positions = jnp.arange(SEQ_LEN)
    causal_mask = positions[:, None] >= positions[None, :]

    def one_head(operands):
        query_h, key_h, value_h = operands
        attn_scores = jnp.dot(query_h, key_h.T, preferred_element_type=jnp.float32) * HEAD_DIM ** -0.5
        attn_scores = jnp.where(causal_mask, attn_scores, -jnp.inf)
        attn_probs = jax.nn.softmax(attn_scores, axis=-1).astype(jnp.bfloat16)
        return jnp.dot(attn_probs, value_h, preferred_element_type=jnp.float32).astype(jnp.bfloat16)

    context = lax.map(one_head, (heads_first[0], heads_first[1], heads_first[2]))
    context = context.reshape(GROUP_BATCH, NUM_HEADS, SEQ_LEN, HEAD_DIM)
    attn_out = jnp.einsum("bhse,hed->bsd", context.astype(jnp.float32), w_out.astype(jnp.float32))
    resid_out = (embed.astype(jnp.float32) + attn_out + b_out).astype(jnp.bfloat16)
    return resid_out, embed
```

```python
import functools
import jax
import jax.numpy as jnp
from jax import lax
from jax.experimental import pallas as pl
from jax.experimental.pallas import tpu as pltpu
from jax.sharding import PartitionSpec as P

LN_EPS = 1e-5
SLOTS = 64
VMEM_LIMIT = 60 * 1024 * 1024
MESH = pl.DeviceIdType.MESH


def layer_norm(values, gain, bias):
    feat_mean = jnp.mean(values, axis=-1, keepdims=True)
    centered = values - feat_mean
    feat_variance = jnp.mean(centered * centered, axis=-1, keepdims=True)
    return centered * lax.rsqrt(feat_variance + LN_EPS) * gain + bias


def vmem():
    return pl.BlockSpec(memory_space=pltpu.VMEM)


def greet(peers):
    barrier = pltpu.get_barrier_semaphore()
    for peer in peers:
        pl.semaphore_signal(barrier, inc=1, device_id=peer, device_id_type=MESH)
    pl.semaphore_wait(barrier, len(peers))


def lookup_kernel(n, rows_ref, bias_ref, count_ref, out_ref, bias_out, count_out,
                  send_sem, recv_sem, bsend_sem, brecv_sem, csend_sem, crecv_sem):
    me = lax.axis_index("tp")
    dp = lax.axis_index("dp")
    peers = [(dp, lax.rem(me + k, n)) for k in range(1, n)]
    greet(peers + [(1 - dp, me)])
    count = pltpu.make_async_remote_copy(
        src_ref=count_ref, dst_ref=count_out, send_sem=csend_sem, recv_sem=crecv_sem,
        device_id=(1 - dp, me), device_id_type=MESH)
    count.start()
    copies = []
    for k in range(1, n):
        copies.append(pltpu.make_async_remote_copy(
            src_ref=rows_ref.at[lax.rem(me + k, n)], dst_ref=out_ref.at[me],
            send_sem=send_sem.at[k], recv_sem=recv_sem.at[k],
            device_id=peers[k - 1], device_id_type=MESH))
        copies[-1].start()
    for k in range(1, n):
        copies.append(pltpu.make_async_remote_copy(
            src_ref=bias_ref, dst_ref=bias_out.at[me],
            send_sem=bsend_sem.at[k], recv_sem=brecv_sem.at[k],
            device_id=peers[k - 1], device_id_type=MESH))
        copies[-1].start()
    out_ref[me] = rows_ref[me]
    bias_out[me] = bias_ref[...]
    count.wait()
    for copy in copies:
        copy.wait()


def lookup_exchange(rows, bias, count):
    n = rows.shape[0]
    return pl.pallas_call(
        functools.partial(lookup_kernel, n),
        out_shape=[
            jax.ShapeDtypeStruct(rows.shape, rows.dtype),
            jax.ShapeDtypeStruct((n,) + bias.shape, bias.dtype),
            jax.ShapeDtypeStruct(count.shape, count.dtype),
        ],
        in_specs=[vmem()] * 3,
        out_specs=[vmem()] * 3,
        scratch_shapes=[pltpu.SemaphoreType.DMA((n,))] * 4 + [pltpu.SemaphoreType.DMA] * 2,
        compiler_params=pltpu.CompilerParams(collective_id=0, has_side_effects=True, vmem_limit_bytes=VMEM_LIMIT),
        cost_estimate=pl.CostEstimate(flops=50_000_000_000, bytes_accessed=8_000_000, transcendentals=0),
        name="lookup_exchange",
    )(rows, bias, count)


def sequence_kernel(n, x_ref, out_ref, send_sem, recv_sem, psend_sem, precv_sem):
    me = lax.axis_index("tp")
    dp = lax.axis_index("dp")
    core = lax.rem(me, 2)
    partner = me + 1 - 2 * core
    peers = [lax.rem(me + k, n) for k in range(1, n)]
    greet([(dp, peer) for peer in peers])
    copies = []
    for k in range(1, n):
        peer = peers[k - 1]
        copies.append(pltpu.make_async_remote_copy(
            src_ref=x_ref.at[peer], dst_ref=out_ref.at[me, lax.rem(peer, 2)],
            send_sem=send_sem.at[k], recv_sem=recv_sem.at[k],
            device_id=(dp, peer), device_id_type=MESH))
        copies[-1].start()
    out_ref[me, core] = x_ref[me]
    forwards = [pltpu.make_async_remote_copy(
        src_ref=x_ref.at[me], dst_ref=out_ref.at[me, core],
        send_sem=psend_sem.at[0], recv_sem=precv_sem.at[0],
        device_id=(dp, partner), device_id_type=MESH)]
    forwards[0].start()
    for k in range(1, n):
        copies[k - 1].wait_recv()
        source = lax.rem(me + n - k, n)
        forwards.append(pltpu.make_async_remote_copy(
            src_ref=out_ref.at[source, core], dst_ref=out_ref.at[source, core],
            send_sem=psend_sem.at[k], recv_sem=precv_sem.at[k],
            device_id=(dp, partner), device_id_type=MESH))
        forwards[-1].start()
    for copy in copies:
        copy.wait_send()
    for copy in forwards:
        copy.wait()


def sequence_exchange(x):
    n, rows, width = x.shape
    return pl.pallas_call(
        functools.partial(sequence_kernel, n),
        out_shape=jax.ShapeDtypeStruct((n, 2, rows, width), x.dtype),
        in_specs=[vmem()],
        out_specs=vmem(),
        scratch_shapes=[pltpu.SemaphoreType.DMA((n,))] * 4,
        compiler_params=pltpu.CompilerParams(collective_id=1, has_side_effects=True, vmem_limit_bytes=VMEM_LIMIT),
        cost_estimate=pl.CostEstimate(flops=50_000_000_000, bytes_accessed=8_000_000, transcendentals=0),
        name="sequence_exchange",
    )(x)


def context_kernel(n, x_ref, out_ref, send_sem, recv_sem):
    me = lax.axis_index("tp")
    dp = lax.axis_index("dp")
    peers = [(dp, lax.rem(me + k, n)) for k in range(1, n)]
    greet(peers)
    copies = []
    for k in range(1, n):
        copies.append(pltpu.make_async_remote_copy(
            src_ref=x_ref.at[lax.rem(me + k, n)], dst_ref=out_ref.at[me],
            send_sem=send_sem.at[k], recv_sem=recv_sem.at[k],
            device_id=peers[k - 1], device_id_type=MESH))
        copies[-1].start()
    out_ref[me] = x_ref[me]
    for copy in copies:
        copy.wait()


def context_exchange(x):
    n = x.shape[0]
    return pl.pallas_call(
        functools.partial(context_kernel, n),
        out_shape=jax.ShapeDtypeStruct(x.shape, x.dtype),
        in_specs=[vmem()],
        out_specs=vmem(),
        scratch_shapes=[pltpu.SemaphoreType.DMA((n,))] * 2,
        compiler_params=pltpu.CompilerParams(collective_id=2, has_side_effects=True, vmem_limit_bytes=VMEM_LIMIT),
        cost_estimate=pl.CostEstimate(flops=50_000_000_000, bytes_accessed=8_000_000, transcendentals=0),
        name="context_exchange",
    )(x)


def attention(normed, w_heads, b_heads):
    seq_len = normed.shape[0]
    heads, _, head_dim, _ = w_heads.shape
    projected = jnp.einsum("sd,hced->chse", normed, w_heads, preferred_element_type=jnp.float32)
    projected = (projected + b_heads.transpose(1, 0, 2)[:, :, None, :]).astype(jnp.bfloat16)
    scores = jnp.einsum("hqe,hke->hqk", projected[0], projected[1], preferred_element_type=jnp.float32) * head_dim ** -0.5
    causal_mask = lax.broadcasted_iota(jnp.int32, (seq_len, seq_len), 0) >= lax.broadcasted_iota(jnp.int32, (seq_len, seq_len), 1)
    scores = jnp.where(causal_mask, scores, -jnp.inf)
    probs = jax.nn.softmax(scores, axis=-1).astype(jnp.bfloat16)
    context = jnp.einsum("hqk,hke->qhe", probs, projected[2], preferred_element_type=jnp.float32).astype(jnp.bfloat16)
    return context.reshape(seq_len, heads * head_dim)


def solution(mesh):
    n = mesh.shape["tp"]

    def local_step(token_ids, word_shard, pos_table, ln_gain, ln_bias, w_qkv, b_qkv, w_out, b_out):
        shard_rows, model_dim = word_shard.shape
        batch, seq_len = token_ids.shape
        head_dim = w_qkv.shape[-1]
        block_len = seq_len // n
        tokens = batch * block_len
        me = lax.axis_index("tp")
        core_groups = [[i for i in range(n) if i % 2 == c] for c in range(2)]

        w_heads = lax.all_gather(w_qkv[:, :, 0, :].transpose(1, 2, 0), "tp", axis=0, axis_index_groups=core_groups)
        w_proj = lax.all_gather(w_out[0], "tp", axis=0).reshape(n // 2, 2, head_dim, model_dim)

        blocks = token_ids.reshape(batch, n, block_len).transpose(1, 0, 2).reshape(n, tokens)
        owner = blocks // shard_rows
        order = jnp.arange(tokens)
        earlier = order[:, None] < order[None, :]
        repeated = jnp.any((blocks[:, :, None] == blocks[:, None, :]) & earlier, axis=1)
        lower = jnp.where(repeated, jnp.iinfo(jnp.int32).max, blocks)[:, :, None]
        slot = jnp.sum(((lower >= (owner * shard_rows)[:, None, :]) & (lower < blocks[:, None, :])).astype(jnp.int32), axis=1)
        listed = (owner == me) & ~repeated
        at_slot = listed[:, :, None] & (slot[:, :, None] == jnp.arange(SLOTS))
        send_list = jnp.sum(jnp.where(at_slot, (blocks - me * shard_rows)[:, :, None], 0), axis=1)
        count = jnp.max(slot).astype(jnp.float32) + 1.0

        send_rows = jnp.take(word_shard, send_list.reshape(-1), axis=0, mode="clip").reshape(n, SLOTS, model_dim)
        got_rows, b_all, other_count = lookup_exchange(send_rows, b_qkv[:, 0, :], jnp.full((8, 128), count, jnp.float32))
        my_owner = lax.dynamic_index_in_dim(owner, me, 0, keepdims=False)
        my_slot = lax.dynamic_index_in_dim(slot, me, 0, keepdims=False)

        def from_lists(_):
            index = my_owner * SLOTS + jnp.minimum(my_slot, SLOTS - 1)
            return jnp.take(got_rows.reshape(n * SLOTS, model_dim), index, axis=0, mode="clip")

        def from_all(_):
            local_ids = token_ids - me * shard_rows
            in_shard = (local_ids >= 0) & (local_ids < shard_rows)
            table_rows = jnp.take(word_shard, local_ids, axis=0, mode="clip")
            partial_rows = jnp.where(in_shard[:, :, None], table_rows, jnp.zeros((), jnp.bfloat16))
            return lax.psum_scatter(partial_rows, "tp", scatter_dimension=1, tiled=True).reshape(tokens, model_dim)

        fits = jnp.maximum(count, other_count[0, 0]) <= SLOTS
        block_rows = lax.cond(fits, from_lists, from_all, None).reshape(batch, block_len, model_dim)
        pos_block = lax.dynamic_slice_in_dim(pos_table, me * block_len, block_len, axis=0)
        embed = (block_rows.astype(jnp.float32) + pos_block.astype(jnp.float32)[None]).astype(jnp.bfloat16)
        normed_block = layer_norm(embed.astype(jnp.float32), ln_gain, ln_bias).astype(jnp.bfloat16)

        normed = sequence_exchange(normed_block.reshape(n, tokens // n, model_dim)).reshape(seq_len, model_dim)
        b_heads = lax.dynamic_index_in_dim(b_all.reshape(n // 2, 2, 3, head_dim), lax.rem(me, 2), 1, keepdims=False)
        context = attention(normed, w_heads, b_heads)
        got_context = context_exchange(context.reshape(n, block_len, n // 2 * head_dim))
        got_context = got_context.reshape(batch, 2, block_len, n // 2, head_dim)
        out_block = jnp.einsum("qcshf,hcfd->qsd", got_context, w_proj, preferred_element_type=jnp.float32)
        resid_out = (embed.astype(jnp.float32) + out_block + b_out).astype(jnp.bfloat16)
        return resid_out, embed

    in_specs = (P("dp", None), P("tp", None), P(None, None), P(None), P(None), P(None, None, "tp", None), P(None, "tp", None), P("tp", None, None), P(None))
    out_specs = (P("dp", "tp", None), P("dp", "tp", None))
    return jax.shard_map(local_step, mesh=mesh, in_specs=in_specs, out_specs=out_specs, check_vma=False)
```

```python
import functools
import jax
import jax.numpy as jnp
from jax import lax
from jax.experimental import pallas as pl
from jax.experimental.pallas import tpu as pltpu
from jax.sharding import PartitionSpec as P

LN_EPS = 1e-5
SLOTS = 64
VMEM_LIMIT = 60 * 1024 * 1024
MESH = pl.DeviceIdType.MESH


def layer_norm(values, gain, bias):
    feat_mean = jnp.mean(values, axis=-1, keepdims=True)
    centered = values - feat_mean
    feat_variance = jnp.mean(centered * centered, axis=-1, keepdims=True)
    return centered * lax.rsqrt(feat_variance + LN_EPS) * gain + bias


def vmem():
    return pl.BlockSpec(memory_space=pltpu.VMEM)


def greet(peers):
    barrier = pltpu.get_barrier_semaphore()
    for peer in peers:
        pl.semaphore_signal(barrier, inc=1, device_id=peer, device_id_type=MESH)
    pl.semaphore_wait(barrier, len(peers))


def lookup_kernel(n, rows_ref, bias_ref, count_ref, out_ref, bias_out, count_out,
                  send_sem, recv_sem, bsend_sem, brecv_sem, csend_sem, crecv_sem):
    me = lax.axis_index("tp")
    dp = lax.axis_index("dp")
    peers = [(dp, lax.rem(me + k, n)) for k in range(1, n)]
    greet(peers + [(1 - dp, me)])
    count = pltpu.make_async_remote_copy(
        src_ref=count_ref, dst_ref=count_out, send_sem=csend_sem, recv_sem=crecv_sem,
        device_id=(1 - dp, me), device_id_type=MESH)
    count.start()
    copies = []
    for k in range(1, n):
        copies.append(pltpu.make_async_remote_copy(
            src_ref=rows_ref.at[lax.rem(me + k, n)], dst_ref=out_ref.at[me],
            send_sem=send_sem.at[k], recv_sem=recv_sem.at[k],
            device_id=peers[k - 1], device_id_type=MESH))
        copies[-1].start()
    for k in range(1, n):
        copies.append(pltpu.make_async_remote_copy(
            src_ref=bias_ref, dst_ref=bias_out.at[me],
            send_sem=bsend_sem.at[k], recv_sem=brecv_sem.at[k],
            device_id=peers[k - 1], device_id_type=MESH))
        copies[-1].start()
    out_ref[me] = rows_ref[me]
    bias_out[me] = bias_ref[...]
    count.wait()
    for copy in copies:
        copy.wait()


def lookup_exchange(rows, bias, count):
    n = rows.shape[0]
    return pl.pallas_call(
        functools.partial(lookup_kernel, n),
        out_shape=[
            jax.ShapeDtypeStruct(rows.shape, rows.dtype),
            jax.ShapeDtypeStruct((n,) + bias.shape, bias.dtype),
            jax.ShapeDtypeStruct(count.shape, count.dtype),
        ],
        in_specs=[vmem()] * 3,
        out_specs=[vmem()] * 3,
        scratch_shapes=[pltpu.SemaphoreType.DMA((n,))] * 4 + [pltpu.SemaphoreType.DMA] * 2,
        compiler_params=pltpu.CompilerParams(collective_id=0, has_side_effects=True, vmem_limit_bytes=VMEM_LIMIT),
        cost_estimate=pl.CostEstimate(flops=50_000_000_000, bytes_accessed=8_000_000, transcendentals=0),
        name="lookup_exchange",
    )(rows, bias, count)


def attend_kernel(n, heads, head_dim, x_ref, w_ref, bias_ref, out_ref, tok, w_all, qkv, ctx, acc,
                  send_sem, recv_sem, psend_sem, precv_sem, csend_sem, crecv_sem, w_sem):
    me = lax.axis_index("tp")
    dp = lax.axis_index("dp")
    core = lax.rem(me, 2)
    plane = me // 4
    partner = me + 1 - 2 * core
    rows, width = x_ref.shape[1:]
    pad = 128
    group = 4 * head_dim
    q_rows = 4 * 2 * rows

    loads = []
    for h in range(heads):
        for part, start in ((0, h * pad), (1, (heads + h) * pad), (2, 2 * heads * pad + h * head_dim)):
            loads.append(pltpu.make_async_copy(w_ref.at[h, part], w_all.at[pl.ds(start, head_dim)], w_sem.at[3 * h + part]))
            loads[-1].start()
    for h in range(2 * heads):
        w_all[pl.ds(h * pad + head_dim, pad - head_dim), :] = jnp.zeros((pad - head_dim, width), w_all.dtype)

    greet([(dp, lax.rem(me + k, n)) for k in range(1, n)])

    def handing(peer, source):
        return pltpu.make_async_remote_copy(
            src_ref=x_ref.at[peer], dst_ref=tok.at[source, lax.rem(peer, 2)],
            send_sem=send_sem.at[peer], recv_sem=recv_sem.at[source],
            device_id=(dp, peer), device_id_type=MESH)

    def sharing(source, side):
        return pltpu.make_async_remote_copy(
            src_ref=tok.at[source, side], dst_ref=tok.at[source, side],
            send_sem=psend_sem.at[source], recv_sem=precv_sem.at[source],
            device_id=(dp, partner), device_id_type=MESH)

    for k in range(1, n):
        handing(lax.rem(me + k, n), me).start()
    tok[me, core] = x_ref[me]
    own = pltpu.make_async_remote_copy(
        src_ref=x_ref.at[me], dst_ref=tok.at[me, core],
        send_sem=psend_sem.at[me], recv_sem=precv_sem.at[me],
        device_id=(dp, partner), device_id_type=MESH)
    own.start()
    for load in loads:
        load.wait()

    def project(z):
        for r in range(4):
            sharing(4 * z + r, 1 - core).wait_recv()
        block = tok[pl.ds(4 * z, 4)].reshape(q_rows, width)
        start = pl.multiple_of(z * q_rows, q_rows)

        def columns(i, _):
            at = pl.ds(pl.multiple_of(i * 256, 256), 256)
            part = lax.dot_general(block, w_all[at, :], (((1,), (1,)), ((), ())), preferred_element_type=jnp.float32)
            qkv[pl.ds(start, q_rows), at] = (part + bias_ref[:, at]).astype(qkv.dtype)
            return 0

        lax.fori_loop(0, w_all.shape[0] // 256, columns, 0)

    for d in range(4):
        z = lax.rem(plane + 4 - d, 4)
        for r in range(4):
            source = 4 * z + r
            if d == 0:
                @pl.when(source != me)
                def _():
                    handing(me, source).wait_recv()
                    sharing(source, core).start()
            else:
                handing(me, source).wait_recv()
                sharing(source, core).start()
        if d:
            project(lax.rem(plane + 5 - d, 4))
    project(lax.rem(plane + 1, 4))

    scale = head_dim ** -0.5 * 1.4426950408889634
    lane_head = lax.broadcasted_iota(jnp.int32, (1, group), 1) // head_dim
    causal = lax.broadcasted_iota(jnp.int32, (q_rows, q_rows), 0) >= lax.broadcasted_iota(jnp.int32, (q_rows, q_rows), 1)

    def delivery(p, source):
        return pltpu.make_async_remote_copy(
            src_ref=ctx.at[p], dst_ref=out_ref.at[source],
            send_sem=csend_sem.at[p], recv_sem=crecv_sem.at[source],
            device_id=(dp, p), device_id_type=MESH)

    for j in (2, 0, 3, 1):
        keys = (j + 1) * q_rows
        done = j * q_rows
        for g in range(heads // 4):
            acc[...] = jnp.zeros_like(acc)

            def one_head(i, _):
                h = 4 * g + i
                q_at = pl.ds(pl.multiple_of(h * pad, pad), pad)
                k_at = pl.ds(pl.multiple_of((heads + h) * pad, pad), pad)
                s = lax.dot_general(qkv[done:keys, q_at], qkv[0:keys, k_at], (((1,), (1,)), ((), ())), preferred_element_type=jnp.float32)
                diagonal = jnp.where(causal, s[:, done:keys], -jnp.inf)
                s = diagonal if j == 0 else jnp.concatenate([s[:, :done], diagonal], axis=1)
                top = jnp.max(s, axis=1, keepdims=True)
                e = jnp.exp2(s * scale - top * scale)
                probs = (e * (1.0 / jnp.sum(e, axis=1, keepdims=True))).astype(jnp.bfloat16)
                v_all = qkv[0:keys, 2 * heads * pad + g * group:2 * heads * pad + (g + 1) * group]
                v = jnp.where(lane_head == i, v_all, jnp.zeros((), v_all.dtype))
                acc[...] += jnp.dot(probs, v, preferred_element_type=jnp.float32)
                return 0

            lax.fori_loop(0, 4, one_head, 0)
            for r in range(4):
                ctx[4 * j + r, :, g * group:(g + 1) * group] = acc[r * 2 * rows:(r + 1) * 2 * rows, :].astype(ctx.dtype)
        for r in range(4):
            p = 4 * j + r

            @pl.when(me != p)
            def _():
                delivery(p, me).start()

            @pl.when(me == p)
            def _():
                out_ref[p] = ctx[p]

    for k in range(1, n):
        peer = lax.rem(me + k, n)
        delivery(peer, me).wait_send()
        delivery(me, peer).wait_recv()
        handing(peer, me).wait_send()
        sharing(peer, core).wait_send()
    own.wait_send()


def attend_exchange(x, w_heads, bias):
    n, rows, width = x.shape
    heads, _, head_dim, _ = w_heads.shape
    block, seq_len, inner, columns = 2 * rows, n * 2 * rows, heads * head_dim, bias.shape[1]
    return pl.pallas_call(
        functools.partial(attend_kernel, n, heads, head_dim),
        out_shape=jax.ShapeDtypeStruct((n, block, inner), x.dtype),
        in_specs=[vmem(), pl.BlockSpec(memory_space=pl.ANY), vmem()],
        out_specs=vmem(),
        scratch_shapes=[
            pltpu.VMEM((n, 2, rows, width), x.dtype),
            pltpu.VMEM((columns, width), x.dtype),
            pltpu.VMEM((seq_len, columns), x.dtype),
            pltpu.VMEM((n, block, inner), x.dtype),
            pltpu.VMEM((4 * block, 4 * head_dim), jnp.float32),
        ] + [pltpu.SemaphoreType.DMA((n,))] * 6 + [pltpu.SemaphoreType.DMA((3 * heads,))],
        compiler_params=pltpu.CompilerParams(collective_id=1, has_side_effects=True, vmem_limit_bytes=VMEM_LIMIT),
        cost_estimate=pl.CostEstimate(flops=50_000_000_000, bytes_accessed=20_000_000, transcendentals=0),
        name="attend_exchange",
    )(x, w_heads, bias)


def solution(mesh):
    n = mesh.shape["tp"]

    def local_step(token_ids, word_shard, pos_table, ln_gain, ln_bias, w_qkv, b_qkv, w_out, b_out):
        shard_rows, model_dim = word_shard.shape
        batch, seq_len = token_ids.shape
        head_dim = w_qkv.shape[-1]
        block_len = seq_len // n
        tokens = batch * block_len
        me = lax.axis_index("tp")
        core_groups = [[i for i in range(n) if i % 2 == c] for c in range(2)]

        w_heads = lax.all_gather(w_qkv[:, :, 0, :].transpose(1, 2, 0), "tp", axis=0, axis_index_groups=core_groups)
        w_proj = lax.all_gather(w_out[0], "tp", axis=0).reshape(n // 2, 2, head_dim, model_dim)

        blocks = token_ids.reshape(batch, n, block_len).transpose(1, 0, 2).reshape(n, tokens)
        owner = blocks // shard_rows
        order = jnp.arange(tokens)
        earlier = order[:, None] < order[None, :]
        repeated = jnp.any((blocks[:, :, None] == blocks[:, None, :]) & earlier, axis=1)
        lower = jnp.where(repeated, jnp.iinfo(jnp.int32).max, blocks)[:, :, None]
        slot = jnp.sum(((lower >= (owner * shard_rows)[:, None, :]) & (lower < blocks[:, None, :])).astype(jnp.int32), axis=1)
        listed = (owner == me) & ~repeated
        my_owner = lax.dynamic_index_in_dim(owner, me, 0, keepdims=False)
        my_slot = lax.dynamic_index_in_dim(slot, me, 0, keepdims=False)

        def rows_to_send(first):
            at_slot = listed[:, :, None] & (slot[:, :, None] == first + jnp.arange(SLOTS))
            send_list = jnp.sum(jnp.where(at_slot, (blocks - me * shard_rows)[:, :, None], 0), axis=1)
            return jnp.take(word_shard, send_list.reshape(-1), axis=0, mode="clip").reshape(n, SLOTS, model_dim)

        def rows_received(got_rows, first):
            index = my_owner * SLOTS + jnp.clip(my_slot - first, 0, SLOTS - 1)
            return jnp.take(got_rows.reshape(n * SLOTS, model_dim), index, axis=0, mode="clip")

        count = jnp.max(slot).astype(jnp.float32) + 1.0
        got_rows, b_all, other_count = lookup_exchange(rows_to_send(0), b_qkv[:, 0, :], jnp.full((8, 128), count, jnp.float32))
        all_count = jnp.maximum(count, other_count[0, 0]).astype(jnp.int32)

        def next_round(carry):
            first, rows = carry
            got = lax.all_to_all(rows_to_send(first), "tp", 0, 0, tiled=True)
            rows = jnp.where((my_slot >= first)[:, None], rows_received(got, first), rows)
            return first + SLOTS, rows

        _, block_rows = lax.while_loop(lambda carry: carry[0] < all_count, next_round, (jnp.int32(SLOTS), rows_received(got_rows, 0)))
        block_rows = block_rows.reshape(batch, block_len, model_dim)
        pos_block = lax.dynamic_slice_in_dim(pos_table, me * block_len, block_len, axis=0)
        embed = (block_rows.astype(jnp.float32) + pos_block.astype(jnp.float32)[None]).astype(jnp.bfloat16)
        normed_block = layer_norm(embed.astype(jnp.float32), ln_gain, ln_bias).astype(jnp.bfloat16)

        b_heads = lax.dynamic_index_in_dim(b_all.reshape(n // 2, 2, 3, head_dim), lax.rem(me, 2), 1, keepdims=False)
        bias_qk = jnp.pad(b_heads[:, :2], ((0, 0), (0, 0), (0, 128 - head_dim))).transpose(1, 0, 2).reshape(1, -1)
        bias = jnp.concatenate([bias_qk, b_heads[:, 2].reshape(1, -1)], axis=1)
        got_context = attend_exchange(normed_block.reshape(n, tokens // n, model_dim), w_heads, bias)
        got_context = got_context.reshape(batch, 2, block_len, n // 2, head_dim)
        out_block = jnp.einsum("qcshf,hcfd->qsd", got_context, w_proj, preferred_element_type=jnp.float32)
        resid_out = (embed.astype(jnp.float32) + out_block + b_out).astype(jnp.bfloat16)
        return resid_out, embed

    in_specs = (P("dp", None), P("tp", None), P(None, None), P(None), P(None), P(None, None, "tp", None), P(None, "tp", None), P("tp", None, None), P(None))
    out_specs = (P("dp", "tp", None), P("dp", "tp", None))

    return jax.shard_map(local_step, mesh=mesh, in_specs=in_specs, out_specs=out_specs, check_vma=False)
```

```python
import functools
import jax
import jax.numpy as jnp
from jax import lax
from jax.experimental import pallas as pl
from jax.experimental.pallas import tpu as pltpu
from jax.sharding import PartitionSpec as P

LN_EPS = 1e-5
SLOTS = 192
LANES = 128
VMEM_LIMIT = 60 * 1024 * 1024
MESH = pl.DeviceIdType.MESH


def layer_norm(values, gain, bias):
    feat_mean = jnp.mean(values, axis=-1, keepdims=True)
    centered = values - feat_mean
    feat_variance = jnp.mean(centered * centered, axis=-1, keepdims=True)
    return centered * lax.rsqrt(feat_variance + LN_EPS) * gain + bias


def vmem():
    return pl.BlockSpec(memory_space=pltpu.VMEM)


def greet(peers):
    barrier = pltpu.get_barrier_semaphore()
    for peer in peers:
        pl.semaphore_signal(barrier, inc=1, device_id=peer, device_id_type=MESH)
    pl.semaphore_wait(barrier, len(peers))


def lookup_kernel(n, rows_ref, note_ref, w_ref, out_ref, notes_out, w_out, zsend, ysend, psend, recv, nsend, nrecv,
                  up_sem, down_sem, side_sem, head_recv, value_recv):
    me = lax.axis_index("tp")
    dp = lax.axis_index("dp")
    plane = me // 4
    chip = me // 2
    core = lax.rem(me, 2)
    partner = me + 1 - 2 * core
    across = me + 2 - 4 * lax.rem(chip, 2)
    far_chip = across // 2
    planes = n // 4
    others = [(dp, lax.rem(me + k, n)) for k in range(1, n)] + [(1 - dp, lax.rem(me + k, n)) for k in range(n)]
    greet(others)

    def line(dz, source, target):
        z = lax.rem(plane + dz, 4)
        return pltpu.make_async_remote_copy(
            src_ref=rows_ref.at[z], dst_ref=out_ref.at[source], send_sem=zsend.at[dz], recv_sem=recv.at[source],
            device_id=(dp, target), device_id_type=MESH)

    def relay(source, target, sem):
        return pltpu.make_async_remote_copy(
            src_ref=out_ref.at[source], dst_ref=out_ref.at[source], send_sem=sem, recv_sem=recv.at[source],
            device_id=(dp, target), device_id_type=MESH)

    def head_part(values, head):
        return w_out.at[head, pl.ds(2, 1)] if values else w_out.at[head, pl.ds(0, 2)]

    def pass_on(values, head, target, sem, first=None):
        part = head_part(values, head)
        source = part if first is None else (w_ref.at[pl.ds(2, 1)] if values else w_ref.at[pl.ds(0, 2)])
        return pltpu.make_async_remote_copy(
            src_ref=source, dst_ref=part, send_sem=sem, recv_sem=(value_recv if values else head_recv).at[head],
            device_id=(dp, target), device_id_type=MESH)

    def along(values, d, side, first=None):
        base = far_chip if side else chip
        kind = 8 * values + 4 * side
        return [
            (jnp.logical_and(plane >= d, plane < planes - 1), lax.rem(base + n // 2 - 2 * d, n // 2), lax.rem(me + 4, n), up_sem.at[kind + d]),
            (jnp.logical_and(plane < planes - d, plane > 0), lax.rem(base + 2 * d, n // 2), lax.rem(me + n - 4, n), down_sem.at[kind + d]),
        ]

    def go(values, d, side, first=None):
        for here, head, target, sem in along(values, d, side):
            @pl.when(here)
            def _():
                pass_on(values, head, target, sem, first).start()

    def arrivals(values, d, side):
        base = far_chip if side else chip
        return [
            (plane >= d, lax.rem(base + n // 2 - 2 * d, n // 2)),
            (plane < planes - d, lax.rem(base + 2 * d, n // 2)),
        ]

    go(False, 0, False, first=True)
    pass_on(True, chip, across, side_sem.at[0], True).start()
    go(True, 0, False, first=True)
    pass_on(False, chip, across, side_sem.at[1], True).start()
    line(2, me, lax.rem(me + 8, n)).start()
    own = []
    for target, sem in ((across, ysend.at[0]), (partner, psend.at[0])):
        own.append(pltpu.make_async_remote_copy(
            src_ref=rows_ref.at[plane], dst_ref=out_ref.at[me], send_sem=sem, recv_sem=recv.at[me],
            device_id=(dp, target), device_id_type=MESH))
        own[-1].start()
    notes = []
    for k, target in enumerate(others):
        notes.append(pltpu.make_async_remote_copy(
            src_ref=note_ref, dst_ref=notes_out.at[dp, me], send_sem=nsend.at[k], recv_sem=nrecv.at[k],
            device_id=target, device_id_type=MESH))
        notes[-1].start()
    out_ref[me] = rows_ref[plane]
    notes_out[dp, me] = note_ref[...]
    w_out[chip] = w_ref[...]

    pass_on(True, far_chip, across, side_sem.at[0]).wait_recv()
    go(True, 0, True)
    line(1, me, lax.rem(me + 4, n)).start()
    line(3, me, lax.rem(me + 12, n)).start()

    def across_heads(d):
        for here, head in arrivals(False, d, False):
            @pl.when(here)
            def _():
                pass_on(False, head, across, side_sem.at[2 + head]).start()

    for d in range(1, planes):
        for here, head in arrivals(False, d, False):
            @pl.when(here)
            def _():
                pass_on(False, head, across, side_sem.at[2 + head]).wait_recv()
        if d < planes - 1:
            go(False, d, False)
        across_heads(d)
        for side in (False, True):
            for here, head in arrivals(True, d, side):
                @pl.when(here)
                def _():
                    pass_on(True, head, across, side_sem.at[0]).wait_recv()
            if d < planes - 1:
                go(True, d, side)
        source = lax.rem(me + n - 4 * d, n)
        line(d, source, me).wait_recv()
        relay(source, across, ysend.at[d]).start()
        relay(source, partner, psend.at[d]).start()
    for d in range(planes):
        source = lax.rem(across + n - 4 * d, n)
        relay(source, across, ysend.at[d]).wait_recv()
        relay(source, partner, psend.at[4 + d]).start()
    for d in range(planes):
        pass_on(False, lax.rem(far_chip + 2 * d, n // 2), across, side_sem.at[1]).wait_recv()
        for from_core in (partner, partner + across - me):
            relay(lax.rem(from_core + n - 4 * d, n), partner, psend.at[d]).wait_recv()

    for copy in own:
        copy.wait_send()
    for d in range(planes):
        source = lax.rem(across + n - 4 * d, n)
        relay(source, partner, psend.at[4 + d]).wait_send()
        if d:
            line(d, me, me).wait_send()
            relay(me, across, ysend.at[d]).wait_send()
            relay(me, partner, psend.at[d]).wait_send()
            for here, head in arrivals(False, d, False):
                @pl.when(here)
                def _():
                    pass_on(False, head, across, side_sem.at[2 + head]).wait_send()
        if d < planes - 1:
            for values, side in ((False, False), (True, False), (True, True)):
                for here, head, target, sem in along(values, d, side):
                    @pl.when(here)
                    def _():
                        pass_on(values, head, target, sem).wait_send()
    pass_on(True, chip, across, side_sem.at[0]).wait_send()
    pass_on(False, chip, across, side_sem.at[1]).wait_send()
    for copy in notes:
        copy.wait()


def lookup_exchange(n, rows, note, w):
    return pl.pallas_call(
        functools.partial(lookup_kernel, n),
        out_shape=[
            jax.ShapeDtypeStruct((n,) + rows.shape[1:], rows.dtype),
            jax.ShapeDtypeStruct((2, n) + note.shape, note.dtype),
            jax.ShapeDtypeStruct((n // 2,) + w.shape, w.dtype),
        ],
        in_specs=[vmem()] * 3,
        out_specs=[vmem()] * 3,
        scratch_shapes=[pltpu.SemaphoreType.DMA((size,)) for size in (4, 4, 8, n, 2 * n, 2 * n, 16, 16, 2 + n // 2, n // 2, n // 2)],
        compiler_params=pltpu.CompilerParams(collective_id=0, has_side_effects=True, vmem_limit_bytes=VMEM_LIMIT),
        cost_estimate=pl.CostEstimate(flops=50_000_000_000, bytes_accessed=8_000_000, transcendentals=0),
        name="lookup_exchange",
    )(rows, note, w)


def attend_kernel(n, heads, head_dim, got_ref, at_ref, pos_seq_ref, pos_own_ref, gain_ref, beta_ref, w_ref, bias_ref,
                  wo_ref, out_ref, embed_ref, proj_ref, tok, w_all, qkv, ctx, acc, psend_sem, precv_sem, csend_sem, crecv_sem, osend_sem, orecv_sem, w_sem):
    me = lax.axis_index("tp")
    dp = lax.axis_index("dp")
    core = lax.rem(me, 2)
    partner = me + 1 - 2 * core
    total_rows, width = got_ref.shape
    half = pos_seq_ref.shape[0]
    block = pos_own_ref.shape[0]
    batch = embed_ref.shape[0]
    pad = LANES
    group = 4 * head_dim
    q_rows = 4 * block
    step = 256

    loads = []
    for h in range(heads):
        for part, start in ((0, h * pad), (1, (heads + h) * pad), (2, 2 * heads * pad + h * head_dim)):
            loads.append(pltpu.make_async_copy(w_ref.at[h, part], w_all.at[pl.ds(start, head_dim)], w_sem.at[3 * h + part]))
            loads[-1].start()
    for h in range(2 * heads):
        w_all[pl.ds(h * pad + head_dim, pad - head_dim), :] = jnp.zeros((pad - head_dim, width), w_all.dtype)
    greet([(dp, lax.rem(me + k, n)) for k in range(1, n)])

    across = me + 2 - 4 * lax.rem(me // 2, 2)

    def spread(source, target, sem, first=False):
        return pltpu.make_async_remote_copy(
            src_ref=wo_ref if first else proj_ref.at[source], dst_ref=proj_ref.at[source],
            send_sem=osend_sem.at[sem], recv_sem=orecv_sem.at[source], device_id=(dp, target), device_id_type=MESH)

    for d in (2, 1, 3):
        spread(me, lax.rem(me + 4 * d, n), 4 * d, True).start()
    for i, target in enumerate((across, partner)):
        spread(me, target, 1 + i, True).start()
    proj_ref[me] = wo_ref[...]

    def table_rows(start, size):
        hit = at_ref[pl.ds(pl.multiple_of(start, 64), size), :] == lax.broadcasted_iota(jnp.int32, (size, total_rows), 1)
        return jnp.dot(hit.astype(jnp.bfloat16), got_ref[...], preferred_element_type=jnp.float32)

    def share(t):
        at = pl.ds(pl.multiple_of(core * half + t * step, step), step)
        return pltpu.make_async_remote_copy(
            src_ref=tok.at[at], dst_ref=tok.at[at], send_sem=psend_sem.at[t], recv_sem=precv_sem.at[t],
            device_id=(dp, partner), device_id_type=MESH)

    steps = half // step

    def embed_step(t, _):
        at = pl.ds(pl.multiple_of(t * step, step), step)
        rows = table_rows(t * step, step) + pos_seq_ref[at, :].astype(jnp.float32)
        values = rows.astype(jnp.bfloat16).astype(jnp.float32)
        tok[pl.ds(pl.multiple_of(core * half + t * step, step), step), :] = layer_norm(values, gain_ref[...], beta_ref[...]).astype(tok.dtype)
        @pl.when(t > 0)
        def _():
            share(t - 1).start()
        return 0

    lax.fori_loop(0, steps, embed_step, 0)
    for load in loads:
        load.wait()

    def project(t, _):
        @pl.when(t >= steps)
        def _():
            share(t - steps).wait_recv()
        at_rows = pl.ds(pl.multiple_of(lax.rem(core * half + t * step, 2 * half), step), step)
        def columns(i, _):
            at = pl.ds(pl.multiple_of(i * 256, 256), 256)
            part = lax.dot_general(tok[at_rows, :], w_all[at, :], (((1,), (1,)), ((), ())), preferred_element_type=jnp.float32)
            qkv[at_rows, at] = (part + bias_ref[:, at]).astype(qkv.dtype)
            return 0
        lax.fori_loop(0, w_all.shape[0] // 256, columns, 0)
        @pl.when(t == 0)
        def _():
            share(steps - 1).start()
        return 0

    lax.fori_loop(0, 2 * steps, project, 0)
    for d in range(1, 4):
        source = lax.rem(me + n - 4 * d, n)
        spread(source, source, 4 * d).wait_recv()
        for i, target in enumerate((across, partner)):
            spread(source, target, 4 * d + 1 + i).start()

    scale = head_dim ** -0.5 * 1.4426950408889634
    lane_head = lax.broadcasted_iota(jnp.int32, (1, group), 1) // head_dim
    causal = lax.broadcasted_iota(jnp.int32, (q_rows, q_rows), 0) >= lax.broadcasted_iota(jnp.int32, (q_rows, q_rows), 1)

    def delivery(p, source):
        return pltpu.make_async_remote_copy(
            src_ref=ctx.at[p], dst_ref=out_ref.at[source],
            send_sem=csend_sem.at[p], recv_sem=crecv_sem.at[source],
            device_id=(dp, p), device_id_type=MESH)

    for turn, j in enumerate((2, 0, 3, 1)):
        keys = (j + 1) * q_rows
        done = j * q_rows

        def head_group(g, _):
            v_at = pl.ds(pl.multiple_of(2 * heads * pad + g * group, pad), group)

            def one_head(i, _):
                h = 4 * g + i
                q = qkv[done:keys, pl.ds(pl.multiple_of(h * pad, pad), pad)]
                k_at = pl.ds(pl.multiple_of((heads + h) * pad, pad), pad)
                nt = (((1,), (1,)), ((), ()))
                near = lax.dot_general(q, qkv[done:keys, k_at], nt, preferred_element_type=jnp.float32)
                near = jnp.where(causal, near, -jnp.inf)
                top = jnp.max(near, axis=1, keepdims=True)
                if j:
                    far = lax.dot_general(q, qkv[0:done, k_at], nt, preferred_element_type=jnp.float32)
                    top = jnp.maximum(top, jnp.max(far, axis=1, keepdims=True))
                top = top * scale
                near = jnp.exp2(near * scale - top)
                total = jnp.sum(near, axis=1, keepdims=True)
                if j:
                    far = jnp.exp2(far * scale - top)
                    total = total + jnp.sum(far, axis=1, keepdims=True)
                part = 1.0 / total
                mine = lane_head == i
                v = jnp.where(mine, qkv[done:keys, v_at], jnp.zeros((), qkv.dtype))
                out = jnp.dot((near * part).astype(jnp.bfloat16), v, preferred_element_type=jnp.float32)
                if j:
                    v = jnp.where(mine, qkv[0:done, v_at], jnp.zeros((), qkv.dtype))
                    out = out + jnp.dot((far * part).astype(jnp.bfloat16), v, preferred_element_type=jnp.float32)
                acc[...] += out
                return 0

            acc[...] = jnp.zeros_like(acc)
            lax.fori_loop(0, 4, one_head, 0)
            for r in range(4):
                ctx[4 * j + r, :, pl.ds(pl.multiple_of(g * group, pad), group)] = acc[r * block:(r + 1) * block, :].astype(ctx.dtype)
            return 0

        lax.fori_loop(0, heads // 4, head_group, 0)
        if turn == 0:
            for d in range(4):
                source = lax.rem(across + n - 4 * d, n)
                spread(source, source, 0).wait_recv()
                spread(source, partner, 4 * d + 3).start()
        for r in range(4):
            p = 4 * j + r
            @pl.when(me != p)
            def _():
                delivery(p, me).start()
            @pl.when(me == p)
            def _():
                out_ref[p] = ctx[p]

    pos_pair = jnp.concatenate([pos_own_ref[...].astype(jnp.float32)] * 2, axis=0)

    def own_step(t, _):
        rows = table_rows(half + t * 2 * block, 2 * block) + pos_pair
        embed_ref[pl.ds(2 * t, 2)] = rows.astype(embed_ref.dtype).reshape(2, block, width)
        return 0

    lax.fori_loop(0, batch // 2, own_step, 0)
    for d in range(4):
        for from_core in (partner, partner + across - me):
            source = lax.rem(from_core + n - 4 * d, n)
            spread(source, source, 0).wait_recv()
    for sem in [1, 2, 3] + [4 * d + i for d in (1, 2, 3) for i in range(4)]:
        spread(me, partner, sem).wait_send()
    for k in range(1, n):
        peer = lax.rem(me + k, n)
        delivery(peer, me).wait_send()
        delivery(me, peer).wait_recv()
    for t in range(half // step):
        share(t).wait_send()


def attend_exchange(n, batch, got, at, pos_seq, pos_own, gain, beta, w_heads, bias, wo):
    heads, _, head_dim, width = w_heads.shape
    block = pos_own.shape[0]
    seq_len, inner, columns = n * block, heads * head_dim, bias.shape[1]
    steps = pos_seq.shape[0] // 256
    return pl.pallas_call(
        functools.partial(attend_kernel, n, heads, head_dim),
        out_shape=[
            jax.ShapeDtypeStruct((n, block, inner), got.dtype),
            jax.ShapeDtypeStruct((batch, block, width), got.dtype),
            jax.ShapeDtypeStruct((n,) + wo.shape, wo.dtype),
        ],
        in_specs=[vmem()] * 6 + [pl.BlockSpec(memory_space=pl.ANY)] + [vmem()] * 2,
        out_specs=[vmem()] * 3,
        scratch_shapes=[
            pltpu.VMEM((seq_len, width), got.dtype),
            pltpu.VMEM((columns, width), got.dtype),
            pltpu.VMEM((seq_len, columns), got.dtype),
            pltpu.VMEM((n, block, inner), got.dtype),
            pltpu.VMEM((4 * block, 4 * head_dim), jnp.float32),
        ] + [pltpu.SemaphoreType.DMA((steps,))] * 2 + [pltpu.SemaphoreType.DMA((n,))] * 4 + [pltpu.SemaphoreType.DMA((3 * heads,))],
        compiler_params=pltpu.CompilerParams(collective_id=1, has_side_effects=True, vmem_limit_bytes=VMEM_LIMIT),
        cost_estimate=pl.CostEstimate(flops=50_000_000_000, bytes_accessed=20_000_000, transcendentals=0),
        name="attend_exchange",
    )(got, at, pos_seq, pos_own, gain, beta, w_heads, bias, wo)


def solution(mesh):
    n = mesh.shape["tp"]

    def local_step(token_ids, word_shard, pos_table, ln_gain, ln_bias, w_qkv, b_qkv, w_out, b_out):
        shard_rows, model_dim = word_shard.shape
        batch, seq_len = token_ids.shape
        head_dim = w_qkv.shape[-1]
        block_len = seq_len // n
        tokens = batch * block_len
        me = lax.axis_index("tp")
        plane_ids = jnp.concatenate([
            token_ids.reshape(batch, 4, seq_len // 4).transpose(1, 0, 2).reshape(4, -1),
            token_ids.reshape(4, -1)], axis=1)
        hi_rows = shard_rows // LANES
        lanes = jnp.arange(LANES)

        def one_hot(hit):
            return hit.astype(jnp.bfloat16)

        def listing(present):
            present = one_hot(present > 0.5)
            in_row = jnp.einsum("...hl,lm->...hm", present, one_hot(lanes[:, None] <= lanes), preferred_element_type=jnp.float32)
            rows = jnp.arange(hi_rows)
            before = jnp.einsum("gh,...h->...g", one_hot(rows[:, None] > rows), in_row[..., -1].astype(jnp.bfloat16), preferred_element_type=jnp.float32)
            return in_row + before[..., None], present.astype(jnp.float32)

        low = one_hot((plane_ids % LANES)[:, :, None] == lanes)
        high = one_hot((plane_ids // LANES - me * hi_rows)[:, None, :] == jnp.arange(hi_rows)[:, None])
        present = jnp.einsum("zht,ztl->zhl", high, low, preferred_element_type=jnp.float32)
        counted, _ = listing(present)
        counted = counted.reshape(4, shard_rows)

        def rows_to_send(first):
            target = (first + jnp.arange(SLOTS)).astype(jnp.float32)
            send_list = jnp.sum((counted[:, None, :] <= target[:, None]).astype(jnp.int32), axis=2)
            return jnp.take(word_shard, send_list.reshape(-1), axis=0, mode="clip").reshape(4, SLOTS, model_dim)

        plane = me // 4
        my_ids = lax.dynamic_index_in_dim(plane_ids, plane, 0, keepdims=False)
        high = one_hot((my_ids // LANES)[None, :] == jnp.arange(n * hi_rows)[:, None])
        low = one_hot((my_ids % LANES)[:, None] == lanes)
        present = jnp.dot(high, low, preferred_element_type=jnp.float32)
        my_counted, my_present = listing(present.reshape(n, hi_rows, LANES))
        slots = (my_counted - my_present).reshape(n * hi_rows, LANES).astype(jnp.int32)
        parts = jnp.concatenate([slots // 64, slots % 64], axis=1).astype(jnp.bfloat16)
        seq_ids = lax.dynamic_slice(token_ids, (me // 2, lax.rem(me, 2) * tokens), (1, tokens))
        own_ids = lax.dynamic_slice_in_dim(token_ids, me * block_len, block_len, axis=1)
        wanted = jnp.concatenate([seq_ids.reshape(-1), own_ids.reshape(-1)])
        found = jnp.dot(one_hot((wanted // LANES)[:, None] == jnp.arange(n * hi_rows)), parts, preferred_element_type=jnp.float32)
        found = jnp.sum(jnp.where(((wanted % LANES)[:, None] == lanes)[:, None, :], found.reshape(-1, 2, LANES), 0.0), axis=2).astype(jnp.int32)
        slot = found[:, 0] * 64 + found[:, 1]
        owner = wanted // shard_rows

        note = jnp.pad(b_qkv[:, 0, :], ((0, 5), (0, LANES - head_dim)))
        note = note.at[3].set(jnp.max(counted))
        got_rows, notes, w_heads = lookup_exchange(n, rows_to_send(0), note, w_qkv[:, :, 0, :].transpose(1, 2, 0))
        got_rows = got_rows.reshape(n * SLOTS, model_dim)
        all_count = jnp.max(notes[:, :, 3, 0]).astype(jnp.int32)

        def fetch_all(carry):
            def next_round(inner):
                first, rows = inner
                send = jnp.broadcast_to(rows_to_send(first)[:, None], (4, n // 4, SLOTS, model_dim)).reshape(n, SLOTS, model_dim)
                got = lax.all_to_all(send, "tp", 0, 0, tiled=True).reshape(n * SLOTS, model_dim)
                picked = jnp.take(got, owner * SLOTS + jnp.clip(slot - first, 0, SLOTS - 1), axis=0, mode="clip")
                return first + SLOTS, jnp.where((slot >= first)[:, None], picked, rows)

            _, rows = lax.while_loop(lambda inner: inner[0] < all_count, next_round, (jnp.int32(0), jnp.zeros((2 * tokens, model_dim), jnp.bfloat16)))
            return jnp.int32(0), jnp.pad(rows, ((0, n * SLOTS - 2 * tokens), (0, 0))), jnp.arange(2 * tokens)

        _, got_rows, row_of = lax.while_loop(lambda carry: carry[0] > SLOTS, fetch_all, (all_count, got_rows, owner * SLOTS + slot))

        b_heads = lax.dynamic_index_in_dim(notes[0, :, :3, :head_dim].reshape(n // 2, 2, 3, head_dim), lax.rem(me, 2), 1, keepdims=False)
        bias_qk = jnp.pad(b_heads[:, :2], ((0, 0), (0, 0), (0, LANES - head_dim))).transpose(1, 0, 2).reshape(1, -1)
        bias = jnp.concatenate([bias_qk, b_heads[:, 2].reshape(1, -1)], axis=1)
        pos_seq = lax.dynamic_slice_in_dim(pos_table, lax.rem(me, 2) * tokens, tokens, axis=0)
        pos_own = lax.dynamic_slice_in_dim(pos_table, me * block_len, block_len, axis=0)
        got_context, embed, w_proj = attend_exchange(n, batch, got_rows, row_of[:, None], pos_seq, pos_own, ln_gain[None], ln_bias[None], w_heads, bias, w_out[0])
        w_proj = w_proj.reshape(n // 2, 2, head_dim, model_dim)
        got_context = got_context.reshape(batch, 2, block_len, n // 2, head_dim)
        out_block = jnp.einsum("qcshf,hcfd->qsd", got_context, w_proj, preferred_element_type=jnp.float32)
        resid_out = (embed.astype(jnp.float32) + out_block + b_out).astype(jnp.bfloat16)
        return resid_out, embed

    in_specs = (P("dp", None), P("tp", None), P(None, None), P(None), P(None), P(None, None, "tp", None), P(None, "tp", None), P("tp", None, None), P(None))
    out_specs = (P("dp", "tp", None), P("dp", "tp", None))
    return jax.shard_map(local_step, mesh=mesh, in_specs=in_specs, out_specs=out_specs, check_vma=False)
```

```python
import functools
import jax
import jax.numpy as jnp
from jax import lax
from jax.experimental import pallas as pl
from jax.experimental.pallas import tpu as pltpu
from jax.sharding import PartitionSpec as P

LN_EPS = 1e-5
SLOTS = 128
LANES = 128
VMEM_LIMIT = 60 * 1024 * 1024
MESH = pl.DeviceIdType.MESH


def layer_norm(values, gain, bias):
    feat_mean = jnp.mean(values, axis=-1, keepdims=True)
    centered = values - feat_mean
    feat_variance = jnp.mean(centered * centered, axis=-1, keepdims=True)
    return centered * lax.rsqrt(feat_variance + LN_EPS) * gain + bias


def vmem():
    return pl.BlockSpec(memory_space=pltpu.VMEM)


def greet(peers):
    barrier = pltpu.get_barrier_semaphore()
    for peer in peers:
        pl.semaphore_signal(barrier, inc=1, device_id=peer, device_id_type=MESH)
    pl.semaphore_wait(barrier, len(peers))


def lookup_kernel(n, rows_ref, note_ref, w_ref, out_ref, notes_out, w_out, transit, zsend, tsend, ysend, psend, recv, trecv, nsend, nrecv,
                  up_sem, down_sem, side_sem, swap_sem, wrecv, xrecv):
    me = lax.axis_index("tp")
    dp = lax.axis_index("dp")
    plane = me // 4
    core = lax.rem(me, 2)
    partner = me + 1 - 2 * core
    across = me + 2 - 4 * lax.rem(me // 2, 2)
    chip = me // 2
    far_chip = across // 2
    planes = n // 4
    part_rows = w_ref.shape[1] // 2
    others = [(dp, lax.rem(me + k, n)) for k in range(1, n)] + [(1 - dp, lax.rem(me + k, n)) for k in range(n)]
    greet(others)

    side = lax.rem(chip, 2)

    def line(dz, source, target):
        return pltpu.make_async_remote_copy(
            src_ref=rows_ref.at[2 * lax.rem(plane + dz, 4) + side], dst_ref=out_ref.at[source],
            send_sem=zsend.at[dz], recv_sem=recv.at[source], device_id=(dp, target), device_id_type=MESH)

    def line_far(dz, target):
        return pltpu.make_async_remote_copy(
            src_ref=rows_ref.at[2 * lax.rem(plane + dz, 4) + 1 - side], dst_ref=transit.at[dz],
            send_sem=tsend.at[dz], recv_sem=trecv.at[dz], device_id=(dp, target), device_id_type=MESH)

    def start_line(dz):
        target = lax.rem(me + 4 * dz, n)
        line_far(dz, target).start()
        line(dz, me, target).start()

    def transfer(dz, source):
        return pltpu.make_async_remote_copy(
            src_ref=transit.at[dz], dst_ref=out_ref.at[source], send_sem=ysend.at[dz], recv_sem=recv.at[source],
            device_id=(dp, across), device_id_type=MESH)

    def relay(source, target, sem):
        return pltpu.make_async_remote_copy(
            src_ref=out_ref.at[source], dst_ref=out_ref.at[source], send_sem=sem, recv_sem=recv.at[source],
            device_id=(dp, target), device_id_type=MESH)

    mine = pl.ds(pl.multiple_of(dp * part_rows, 16), part_rows)

    def pass_on(head, target, sem, first=False):
        part = w_out.at[head, :, mine]
        return pltpu.make_async_remote_copy(
            src_ref=w_ref.at[:, mine] if first else part, dst_ref=part, send_sem=sem, recv_sem=wrecv.at[head],
            device_id=(dp, target), device_id_type=MESH)

    def swap(head):
        part = w_out.at[head, :, mine]
        return pltpu.make_async_remote_copy(
            src_ref=part, dst_ref=part, send_sem=swap_sem.at[head], recv_sem=xrecv.at[head],
            device_id=(1 - dp, me), device_id_type=MESH)

    def along(d):
        return [
            (jnp.logical_and(plane >= d, plane < planes - 1), lax.rem(chip + n // 2 - 2 * d, n // 2), lax.rem(me + 4, n), up_sem.at[d]),
            (jnp.logical_and(plane < planes - d, plane > 0), lax.rem(chip + 2 * d, n // 2), lax.rem(me + n - 4, n), down_sem.at[d]),
        ]

    def arrivals(d, base):
        return [(plane >= d, lax.rem(base + n // 2 - 2 * d, n // 2)), (plane < planes - d, lax.rem(base + 2 * d, n // 2))]

    for here, head, target, sem in along(0):
        @pl.when(here)
        def _():
            pass_on(head, target, sem, True).start()
    pass_on(chip, across, side_sem.at[chip], True).start()
    start_line(2)
    own = []
    for target, of_chip, sem in ((across, far_chip, ysend.at[0]), (partner, chip, psend.at[0])):
        own.append(pltpu.make_async_remote_copy(
            src_ref=rows_ref.at[of_chip], dst_ref=out_ref.at[me], send_sem=sem, recv_sem=recv.at[me],
            device_id=(dp, target), device_id_type=MESH))
        own[-1].start()
    notes = []
    for k, target in enumerate(others):
        notes.append(pltpu.make_async_remote_copy(
            src_ref=note_ref, dst_ref=notes_out.at[dp, me], send_sem=nsend.at[k], recv_sem=nrecv.at[k],
            device_id=target, device_id_type=MESH))
        notes[-1].start()
    out_ref[me] = rows_ref[chip]
    notes_out[dp, me] = note_ref[...]

    w_out[chip] = w_ref[...]

    def near_heads(d):
        for here, head in arrivals(d, chip):
            @pl.when(here)
            def _():
                pass_on(head, across, side_sem.at[head]).wait_recv()
        if d < planes - 1:
            for here, head, target, sem in along(d):
                @pl.when(here)
                def _():
                    pass_on(head, target, sem).start()
        for here, head in arrivals(d, chip):
            @pl.when(here)
            def _():
                pass_on(head, across, side_sem.at[head]).start()
                swap(head).start()

    def far_heads(d):
        for here, head in arrivals(d, far_chip) if d else [(plane >= 0, far_chip)]:
            @pl.when(here)
            def _():
                pass_on(head, across, side_sem.at[0]).wait_recv()
                swap(head).start()

    def near_rows(d):
        source = lax.rem(me + n - 4 * d, n)
        line_far(d, across).wait_recv()
        transfer(d, source).start()
        line(d, source, across).wait_recv()
        relay(source, partner, psend.at[d]).start()

    def far_rows(d):
        source = lax.rem(across + n - 4 * d, n)
        relay(source, across, ysend.at[d]).wait_recv()
        relay(source, partner, psend.at[4 + d]).start()

    near_heads(1)
    start_line(1)
    start_line(3)
    far_heads(0)
    near_rows(2)
    far_rows(0)
    near_heads(2)
    far_heads(1)
    near_rows(1)
    near_rows(3)
    far_rows(2)
    near_heads(3)
    far_heads(2)
    far_rows(1)
    far_rows(3)
    far_heads(3)
    for d in range(planes):
        for from_core in (partner, partner + across - me):
            relay(lax.rem(from_core + n - 4 * d, n), partner, psend.at[d]).wait_recv()

    for copy in own:
        copy.wait_send()
    pass_on(chip, across, side_sem.at[chip]).wait_send()
    for d in range(planes):
        relay(me, partner, psend.at[4 + d]).wait_send()
        if d:
            line(d, me, across).wait_send()
            line_far(d, across).wait_send()
            transfer(d, me).wait_send()
            relay(me, partner, psend.at[d]).wait_send()
            for here, head in arrivals(d, chip):
                @pl.when(here)
                def _():
                    pass_on(head, across, side_sem.at[head]).wait_send()
        if d < planes - 1:
            for here, head, target, sem in along(d):
                @pl.when(here)
                def _():
                    pass_on(head, target, sem).wait_send()
    others_half = pl.ds(pl.multiple_of((1 - dp) * part_rows, 16), part_rows)
    for k in range(1, n // 2):
        head = lax.rem(chip + k, n // 2)
        swap(head).wait_send()
        pltpu.make_async_remote_copy(
            src_ref=w_out.at[head, :, others_half], dst_ref=w_out.at[head, :, others_half],
            send_sem=swap_sem.at[head], recv_sem=xrecv.at[head],
            device_id=(1 - dp, me), device_id_type=MESH).wait_recv()
    for copy in notes:
        copy.wait()


def lookup_exchange(n, rows, note, w):
    return pl.pallas_call(
        functools.partial(lookup_kernel, n),
        out_shape=[
            jax.ShapeDtypeStruct((n,) + rows.shape[1:], rows.dtype),
            jax.ShapeDtypeStruct((2, n) + note.shape, note.dtype),
            jax.ShapeDtypeStruct((n // 2,) + w.shape, w.dtype),
        ],
        in_specs=[vmem()] * 3,
        out_specs=[vmem()] * 3,
        scratch_shapes=[pltpu.VMEM((4,) + rows.shape[1:], rows.dtype)] + [pltpu.SemaphoreType.DMA((size,)) for size in (4, 4, 4, 8, n, 4, 2 * n, 2 * n, 4, 4, n // 2, n // 2, n // 2, n // 2)],
        compiler_params=pltpu.CompilerParams(collective_id=0, has_side_effects=True, vmem_limit_bytes=VMEM_LIMIT),
        cost_estimate=pl.CostEstimate(flops=50_000_000_000, bytes_accessed=8_000_000, transcendentals=0),
        name="lookup_exchange",
    )(rows, note, w)


def attend_kernel(n, heads, head_dim, got_ref, at_ref, pos_ref, gain_ref, beta_ref, w_ref, bias_ref, wo_ref,
                  out_ref, embed_ref, proj_ref, tok, w_all, qkv, ctx, acc, pos_seq, pos_own, psend_sem, precv_sem,
                  csend_sem, crecv_sem, osend_sem, orecv_sem, load_sem):
    me = lax.axis_index("tp")
    dp = lax.axis_index("dp")
    core = lax.rem(me, 2)
    chip = me // 2
    side = lax.rem(chip, 2)
    partner = me + 1 - 2 * core
    across = me + 2 - 4 * side
    total_rows, width = got_ref.shape
    half, block = pos_seq.shape[0], pos_own.shape[0]
    batch = embed_ref.shape[0]
    pad = LANES
    group = 4 * head_dim
    q_rows = 4 * block
    step = 256
    steps = half // step

    loads = [
        pltpu.make_async_copy(pos_ref.at[pl.ds(pl.multiple_of(core * half, 32), half)], pos_seq, load_sem.at[3 * heads]),
        pltpu.make_async_copy(pos_ref.at[pl.ds(pl.multiple_of(me * block, 32), block)], pos_own, load_sem.at[3 * heads + 1])]
    for head in range(heads):
        for part in range(3):
            start = 2 * heads * pad + head * head_dim if part == 2 else (part * heads + head) * pad
            loads.append(pltpu.make_async_copy(w_ref.at[head, part], w_all.at[pl.ds(start, head_dim)], load_sem.at[3 * head + part]))
    for load in loads:
        load.start()
    for h in range(2 * heads):
        w_all[pl.ds(h * pad + head_dim, pad - head_dim), :] = jnp.zeros((pad - head_dim, width), w_all.dtype)
    greet([(dp, lax.rem(me + k, n)) for k in range(1, n)])
    for load in loads[:2]:
        load.wait()

    def proj_at(source):
        return proj_ref.at[lax.rem(source, 2) * (n // 2) + source // 2]

    def spread(source, target, sem, first=False):
        return pltpu.make_async_remote_copy(
            src_ref=wo_ref if first else proj_at(source), dst_ref=proj_at(source),
            send_sem=osend_sem.at[sem], recv_sem=orecv_sem.at[source], device_id=(dp, target), device_id_type=MESH)

    for d in (2, 1, 3):
        spread(me, lax.rem(me + 4 * d, n), 4 * d, True).start()
    for i, target in enumerate((across, partner)):
        spread(me, target, 1 + i, True).start()
    proj_ref[core * (n // 2) + chip] = wo_ref[...]

    def table_rows(start, size):
        hit = at_ref[pl.ds(pl.multiple_of(start, 64), size), :] == lax.broadcasted_iota(jnp.int32, (size, total_rows), 1)
        return jnp.dot(hit.astype(jnp.bfloat16), got_ref[...], preferred_element_type=jnp.float32)

    def share(t):
        at = pl.ds(pl.multiple_of(core * half + t * step, step), step)
        return pltpu.make_async_remote_copy(
            src_ref=tok.at[at], dst_ref=tok.at[at], send_sem=psend_sem.at[t], recv_sem=precv_sem.at[t],
            device_id=(dp, partner), device_id_type=MESH)

    def embed_step(t, _):
        at = pl.ds(pl.multiple_of(t * step, step), step)
        rows = table_rows(t * step, step) + pos_seq[at, :].astype(jnp.float32)
        values = rows.astype(jnp.bfloat16).astype(jnp.float32)
        tok[pl.ds(pl.multiple_of(core * half + t * step, step), step), :] = layer_norm(values, gain_ref[...], beta_ref[...]).astype(tok.dtype)
        @pl.when(t > 0)
        def _():
            share(t - 1).start()
        return 0

    lax.fori_loop(0, steps, embed_step, 0)
    for load in loads[2:]:
        load.wait()

    def project(part, _):
        @pl.when(part == 1)
        def _():
            for t in range(steps):
                share(t).wait_recv()
        at_rows = pl.ds(pl.multiple_of(lax.rem(core + part, 2) * half, step), half)

        def columns(i, _):
            at = pl.ds(pl.multiple_of(i * 256, 256), 256)
            out = lax.dot_general(tok[at_rows, :], w_all[at, :], nt, preferred_element_type=jnp.float32)
            qkv[at_rows, at] = (out + bias_ref[:, at]).astype(qkv.dtype)
            @pl.when(jnp.logical_and(part == 0, i == 0))
            def _():
                share(steps - 1).start()
            return 0

        lax.fori_loop(0, w_all.shape[0] // 256, columns, 0)
        return 0

    scale = head_dim ** -0.5 * 1.4426950408889634
    lane_head = lax.broadcasted_iota(jnp.int32, (1, group), 1) // head_dim
    causal = lax.broadcasted_iota(jnp.int32, (q_rows, q_rows), 0) >= lax.broadcasted_iota(jnp.int32, (q_rows, q_rows), 1)
    nt = (((1,), (1,)), ((), ()))

    def delivery(p, source):
        return pltpu.make_async_remote_copy(
            src_ref=ctx.at[p], dst_ref=out_ref.at[source],
            send_sem=csend_sem.at[p], recv_sem=crecv_sem.at[source],
            device_id=(dp, p), device_id_type=MESH)

    lax.fori_loop(0, 2, project, 0)
    for d in range(1, 4):
        source = lax.rem(me + n - 4 * d, n)
        spread(source, across, 0).wait_recv()
        for i, target in enumerate((across, partner)):
            spread(source, target, 4 * d + 1 + i).start()

    for number, j in enumerate((2, 0, 3, 1)):
        keys = (j + 1) * q_rows
        done = j * q_rows

        def head_group(g, _):
            v_at = pl.ds(pl.multiple_of(2 * heads * pad + g * group, pad), group)

            def one_head(i):
                h = 4 * g + i
                q = qkv[done:keys, pl.ds(pl.multiple_of(h * pad, pad), pad)]
                k_at = pl.ds(pl.multiple_of((heads + h) * pad, pad), pad)
                near = lax.dot_general(q, qkv[done:keys, k_at], nt, preferred_element_type=jnp.float32)
                near = jnp.where(causal, near, -jnp.inf)
                top = jnp.max(near, axis=1, keepdims=True)
                if j:
                    far = lax.dot_general(q, qkv[0:done, k_at], nt, preferred_element_type=jnp.float32)
                    top = jnp.maximum(top, jnp.max(far, axis=1, keepdims=True))
                top = top * scale
                near = jnp.exp2(near * scale - top)
                total = jnp.sum(near, axis=1, keepdims=True)
                if j:
                    far = jnp.exp2(far * scale - top)
                    total = total + jnp.sum(far, axis=1, keepdims=True)
                part = 1.0 / total
                mine = lane_head == i
                v = jnp.where(mine, qkv[done:keys, v_at], jnp.zeros((), qkv.dtype))
                out = jnp.dot((near * part).astype(jnp.bfloat16), v, preferred_element_type=jnp.float32)
                if j:
                    v = jnp.where(mine, qkv[0:done, v_at], jnp.zeros((), qkv.dtype))
                    out = out + jnp.dot((far * part).astype(jnp.bfloat16), v, preferred_element_type=jnp.float32)
                acc[...] += out

            def two_heads(i, _):
                one_head(2 * i)
                one_head(2 * i + 1)
                return 0

            acc[...] = jnp.zeros_like(acc)
            lax.fori_loop(0, 2, two_heads, 0)
            for r in range(4):
                ctx[4 * j + r, :, pl.ds(pl.multiple_of(g * group, pad), group)] = acc[r * block:(r + 1) * block, :].astype(ctx.dtype)
            return 0

        lax.fori_loop(0, heads // 4, head_group, 0)
        for r in range(4):
            p = 4 * j + r
            @pl.when(me != p)
            def _():
                delivery(p, me).start()
        if number == 1:
            for d in range(4):
                source = lax.rem(across + n - 4 * d, n)
                spread(source, across, 0).wait_recv()
                spread(source, partner, 4 * d + 3).start()

    out_ref[me] = ctx[me]
    pos_pair = jnp.concatenate([pos_own[...].astype(jnp.float32)] * 2, axis=0)

    def own_step(t, _):
        rows = table_rows(half + t * 2 * block, 2 * block) + pos_pair
        embed_ref[pl.ds(2 * t, 2)] = rows.astype(embed_ref.dtype).reshape(2, block, width)
        return 0

    lax.fori_loop(0, batch // 2, own_step, 0)
    for d in range(4):
        for from_core in (partner, partner + across - me):
            spread(lax.rem(from_core + n - 4 * d, n), partner, 0).wait_recv()
    for sem in [1, 2, 3] + [4 * d + i for d in (1, 2, 3) for i in range(4)]:
        spread(me, partner, sem).wait_send()
    for k in range(1, n):
        peer = lax.rem(me + k, n)
        delivery(peer, me).wait_send()
        delivery(me, peer).wait_recv()
    for t in range(steps):
        share(t).wait_send()


def attend_exchange(n, batch, got, at, pos, gain, beta, w, bias, wo):
    heads, _, head_dim, width = w.shape
    seq_len = pos.shape[0]
    block, inner, columns = seq_len // n, heads * head_dim, bias.shape[1]
    steps = seq_len // 2 // 256
    hbm = pl.BlockSpec(memory_space=pl.ANY)
    return pl.pallas_call(
        functools.partial(attend_kernel, n, heads, head_dim),
        out_shape=[
            jax.ShapeDtypeStruct((n, block, inner), got.dtype),
            jax.ShapeDtypeStruct((batch, block, width), got.dtype),
            jax.ShapeDtypeStruct((n,) + wo.shape, wo.dtype),
        ],
        in_specs=[vmem(), vmem(), hbm, vmem(), vmem(), hbm, vmem(), vmem()],
        out_specs=[vmem()] * 3,
        scratch_shapes=[
            pltpu.VMEM((seq_len, width), got.dtype),
            pltpu.VMEM((columns, width), got.dtype),
            pltpu.VMEM((seq_len, columns), got.dtype),
            pltpu.VMEM((n, block, inner), got.dtype),
            pltpu.VMEM((4 * block, 4 * head_dim), jnp.float32),
            pltpu.VMEM((seq_len // 2, width), got.dtype),
            pltpu.VMEM((block, width), got.dtype),
        ] + [pltpu.SemaphoreType.DMA((size,)) for size in (steps, steps, n, n, n, n, 3 * heads + 2)],
        compiler_params=pltpu.CompilerParams(collective_id=1, has_side_effects=True, vmem_limit_bytes=VMEM_LIMIT),
        cost_estimate=pl.CostEstimate(flops=50_000_000_000, bytes_accessed=20_000_000, transcendentals=0),
        name="attend_exchange",
    )(got, at, pos, gain, beta, w, bias, wo)


def solution(mesh):
    n = mesh.shape["tp"]

    def local_step(token_ids, word_shard, pos_table, ln_gain, ln_bias, w_qkv, b_qkv, w_out, b_out):
        shard_rows, model_dim = word_shard.shape
        batch, seq_len = token_ids.shape
        head_dim = w_qkv.shape[-1]
        block_len = seq_len // n
        tokens = batch * block_len
        me = lax.axis_index("tp")
        chips = n // 2
        chip_ids = jnp.concatenate([
            token_ids.reshape(batch, chips, 2 * block_len).transpose(1, 0, 2).reshape(chips, -1),
            token_ids], axis=1)
        hi_rows = shard_rows // LANES
        lanes = jnp.arange(LANES)

        def one_hot(hit):
            return hit.astype(jnp.bfloat16)

        def listing(present):
            present = one_hot(present > 0.5)
            in_row = jnp.einsum("...hl,lm->...hm", present, one_hot(lanes[:, None] <= lanes), preferred_element_type=jnp.float32)
            rows = jnp.arange(hi_rows)
            before = jnp.einsum("gh,...h->...g", one_hot(rows[:, None] > rows), in_row[..., -1].astype(jnp.bfloat16), preferred_element_type=jnp.float32)
            return in_row + before[..., None], present.astype(jnp.float32)

        low = one_hot((chip_ids % LANES)[:, :, None] == lanes)
        high = one_hot((chip_ids // LANES - me * hi_rows)[:, None, :] == jnp.arange(hi_rows)[:, None])
        present = jnp.einsum("zht,ztl->zhl", high, low, preferred_element_type=jnp.float32)
        counted, _ = listing(present)
        counted = counted.reshape(chips, shard_rows)

        def rows_to_send(first):
            target = (first + jnp.arange(SLOTS)).astype(jnp.float32)
            send_list = jnp.sum((counted[:, None, :] <= target[:, None]).astype(jnp.int32), axis=2)
            return jnp.take(word_shard, send_list.reshape(-1), axis=0, mode="clip").reshape(chips, SLOTS, model_dim)

        my_ids = lax.dynamic_index_in_dim(chip_ids, me // 2, 0, keepdims=False)
        high = one_hot((my_ids // LANES)[None, :] == jnp.arange(n * hi_rows)[:, None])
        low = one_hot((my_ids % LANES)[:, None] == lanes)
        present = jnp.dot(high, low, preferred_element_type=jnp.float32)
        my_counted, my_present = listing(present.reshape(n, hi_rows, LANES))
        slots = (my_counted - my_present).reshape(n * hi_rows, LANES).astype(jnp.int32)
        parts = jnp.concatenate([slots // 64, slots % 64], axis=1).astype(jnp.bfloat16)
        seq_ids = lax.dynamic_slice(token_ids, (me // 2, lax.rem(me, 2) * tokens), (1, tokens))
        own_ids = lax.dynamic_slice_in_dim(token_ids, me * block_len, block_len, axis=1)
        wanted = jnp.concatenate([seq_ids.reshape(-1), own_ids.reshape(-1)])
        found = jnp.dot(one_hot((wanted // LANES)[:, None] == jnp.arange(n * hi_rows)), parts, preferred_element_type=jnp.float32)
        found = jnp.sum(jnp.where(((wanted % LANES)[:, None] == lanes)[:, None, :], found.reshape(-1, 2, LANES), 0.0), axis=2).astype(jnp.int32)
        slot = found[:, 0] * 64 + found[:, 1]
        owner = wanted // shard_rows

        note = jnp.pad(b_qkv[:, 0, :], ((0, 5), (0, LANES - head_dim)))
        note = note.at[3].set(jnp.max(counted))
        w_own = w_qkv[:, :, 0, :].transpose(1, 2, 0)
        got_rows, notes, w_heads = lookup_exchange(n, rows_to_send(0), note, w_own)
        got_rows = got_rows.reshape(n * SLOTS, model_dim)
        all_count = jnp.max(notes[:, :, 3, 0]).astype(jnp.int32)

        def fetch_all(carry):
            def next_round(inner):
                first, rows = inner
                send = jnp.broadcast_to(rows_to_send(first)[:, None], (chips, 2, SLOTS, model_dim)).reshape(n, SLOTS, model_dim)
                got = lax.all_to_all(send, "tp", 0, 0, tiled=True).reshape(n * SLOTS, model_dim)
                picked = jnp.take(got, owner * SLOTS + jnp.clip(slot - first, 0, SLOTS - 1), axis=0, mode="clip")
                return first + SLOTS, jnp.where((slot >= first)[:, None], picked, rows)

            _, rows = lax.while_loop(lambda inner: inner[0] < all_count, next_round, (jnp.int32(0), jnp.zeros((2 * tokens, model_dim), jnp.bfloat16)))
            return jnp.int32(0), jnp.pad(rows, ((0, n * SLOTS - 2 * tokens), (0, 0))), jnp.arange(2 * tokens)

        _, got_rows, row_of = lax.while_loop(lambda carry: carry[0] > SLOTS, fetch_all, (all_count, got_rows, owner * SLOTS + slot))

        b_heads = lax.dynamic_index_in_dim(notes[0, :, :3, :head_dim].reshape(n // 2, 2, 3, head_dim), lax.rem(me, 2), 1, keepdims=False)
        bias_qk = jnp.pad(b_heads[:, :2], ((0, 0), (0, 0), (0, LANES - head_dim))).transpose(1, 0, 2).reshape(1, -1)
        bias = jnp.concatenate([bias_qk, b_heads[:, 2].reshape(1, -1)], axis=1)
        got_context, embed, w_proj = attend_exchange(n, batch, got_rows, row_of[:, None], pos_table, ln_gain[None], ln_bias[None], w_heads, bias, w_out[0])
        got_context = got_context.reshape(batch, 2, block_len, n // 2 * head_dim)
        out_block = jnp.einsum("qcsf,cfd->qsd", got_context, w_proj.reshape(2, n // 2 * head_dim, model_dim), preferred_element_type=jnp.float32)
        resid_out = (embed.astype(jnp.float32) + out_block + b_out).astype(jnp.bfloat16)
        return resid_out, embed

    in_specs = (P("dp", None), P("tp", None), P(None, None), P(None), P(None), P(None, None, "tp", None), P(None, "tp", None), P("tp", None, None), P(None))
    out_specs = (P("dp", "tp", None), P("dp", "tp", None))
    return jax.shard_map(local_step, mesh=mesh, in_specs=in_specs, out_specs=out_specs, check_vma=False)
```

```python
import functools
import jax
import jax.numpy as jnp
from jax import lax
from jax.experimental import pallas as pl
from jax.experimental.pallas import tpu as pltpu
from jax.sharding import PartitionSpec as P

LN_EPS = 1e-5
SLOTS = 128
LANES = 128
VMEM_LIMIT = 60 * 1024 * 1024
MESH = pl.DeviceIdType.MESH


def layer_norm(values, gain, bias):
    feat_mean = jnp.mean(values, axis=-1, keepdims=True)
    centered = values - feat_mean
    feat_variance = jnp.mean(centered * centered, axis=-1, keepdims=True)
    return centered * lax.rsqrt(feat_variance + LN_EPS) * gain + bias


def vmem():
    return pl.BlockSpec(memory_space=pltpu.VMEM)


def greet(peers):
    barrier = pltpu.get_barrier_semaphore()
    for peer in peers:
        pl.semaphore_signal(barrier, inc=1, device_id=peer, device_id_type=MESH)
    pl.semaphore_wait(barrier, len(peers))


def lookup_kernel(n, rows_ref, note_ref, w_ref, out_ref, notes_out, w_out, transit, zsend, tsend, ysend, psend, recv, trecv, nsend, nrecv,
                  up_sem, down_sem, side_sem, swap_sem, wrecv, xrecv):
    me = lax.axis_index("tp")
    dp = lax.axis_index("dp")
    plane = me // 4
    core = lax.rem(me, 2)
    partner = me + 1 - 2 * core
    across = me + 2 - 4 * lax.rem(me // 2, 2)
    chip = me // 2
    far_chip = across // 2
    planes = n // 4
    part_rows = w_ref.shape[1] // 2
    others = [(dp, lax.rem(me + k, n)) for k in range(1, n)] + [(1 - dp, lax.rem(me + k, n)) for k in range(n)]
    greet(others)

    side = lax.rem(chip, 2)

    def line(dz, source, target):
        return pltpu.make_async_remote_copy(
            src_ref=rows_ref.at[2 * lax.rem(plane + dz, 4) + side], dst_ref=out_ref.at[source],
            send_sem=zsend.at[dz], recv_sem=recv.at[source], device_id=(dp, target), device_id_type=MESH)

    def line_far(dz, target):
        return pltpu.make_async_remote_copy(
            src_ref=rows_ref.at[2 * lax.rem(plane + dz, 4) + 1 - side], dst_ref=transit.at[dz],
            send_sem=tsend.at[dz], recv_sem=trecv.at[dz], device_id=(dp, target), device_id_type=MESH)

    def start_line(dz):
        target = lax.rem(me + 4 * dz, n)
        line_far(dz, target).start()
        line(dz, me, target).start()

    def transfer(dz, source):
        return pltpu.make_async_remote_copy(
            src_ref=transit.at[dz], dst_ref=out_ref.at[source], send_sem=ysend.at[dz], recv_sem=recv.at[source],
            device_id=(dp, across), device_id_type=MESH)

    def relay(source, target, sem):
        return pltpu.make_async_remote_copy(
            src_ref=out_ref.at[source], dst_ref=out_ref.at[source], send_sem=sem, recv_sem=recv.at[source],
            device_id=(dp, target), device_id_type=MESH)

    mine = pl.ds(pl.multiple_of(dp * part_rows, 16), part_rows)

    def pass_on(head, target, sem, first=False):
        part = w_out.at[head, :, mine]
        return pltpu.make_async_remote_copy(
            src_ref=w_ref.at[:, mine] if first else part, dst_ref=part, send_sem=sem, recv_sem=wrecv.at[head],
            device_id=(dp, target), device_id_type=MESH)

    def swap(head):
        part = w_out.at[head, :, mine]
        return pltpu.make_async_remote_copy(
            src_ref=part, dst_ref=part, send_sem=swap_sem.at[head], recv_sem=xrecv.at[head],
            device_id=(1 - dp, me), device_id_type=MESH)

    def along(d):
        return [
            (jnp.logical_and(plane >= d, plane < planes - 1), lax.rem(chip + n // 2 - 2 * d, n // 2), lax.rem(me + 4, n), up_sem.at[d]),
            (jnp.logical_and(plane < planes - d, plane > 0), lax.rem(chip + 2 * d, n // 2), lax.rem(me + n - 4, n), down_sem.at[d]),
        ]

    def arrivals(d, base):
        return [(plane >= d, lax.rem(base + n // 2 - 2 * d, n // 2)), (plane < planes - d, lax.rem(base + 2 * d, n // 2))]

    for here, head, target, sem in along(0):
        @pl.when(here)
        def _():
            pass_on(head, target, sem, True).start()
    pass_on(chip, across, side_sem.at[chip], True).start()
    start_line(2)
    own = []
    for target, of_chip, sem in ((across, far_chip, ysend.at[0]), (partner, chip, psend.at[0])):
        own.append(pltpu.make_async_remote_copy(
            src_ref=rows_ref.at[of_chip], dst_ref=out_ref.at[me], send_sem=sem, recv_sem=recv.at[me],
            device_id=(dp, target), device_id_type=MESH))
        own[-1].start()
    notes = []
    for k, target in enumerate(others):
        notes.append(pltpu.make_async_remote_copy(
            src_ref=note_ref, dst_ref=notes_out.at[dp, me], send_sem=nsend.at[k], recv_sem=nrecv.at[k],
            device_id=target, device_id_type=MESH))
        notes[-1].start()
    out_ref[me] = rows_ref[chip]
    notes_out[dp, me] = note_ref[...]

    w_out[chip] = w_ref[...]

    def near_heads(d):
        for here, head in arrivals(d, chip):
            @pl.when(here)
            def _():
                pass_on(head, across, side_sem.at[head]).wait_recv()
        if d < planes - 1:
            for here, head, target, sem in along(d):
                @pl.when(here)
                def _():
                    pass_on(head, target, sem).start()
        for here, head in arrivals(d, chip):
            @pl.when(here)
            def _():
                pass_on(head, across, side_sem.at[head]).start()
                swap(head).start()

    def far_heads(d):
        for here, head in arrivals(d, far_chip) if d else [(plane >= 0, far_chip)]:
            @pl.when(here)
            def _():
                pass_on(head, across, side_sem.at[0]).wait_recv()
                swap(head).start()

    def near_rows(d):
        source = lax.rem(me + n - 4 * d, n)
        line_far(d, across).wait_recv()
        transfer(d, source).start()
        line(d, source, across).wait_recv()
        relay(source, partner, psend.at[d]).start()

    def far_rows(d):
        source = lax.rem(across + n - 4 * d, n)
        relay(source, across, ysend.at[d]).wait_recv()
        relay(source, partner, psend.at[4 + d]).start()

    near_heads(1)
    start_line(1)
    start_line(3)
    far_heads(0)
    near_rows(2)
    far_rows(0)
    near_heads(2)
    far_heads(1)
    near_rows(1)
    near_rows(3)
    far_rows(2)
    near_heads(3)
    far_heads(2)
    far_rows(1)
    far_rows(3)
    far_heads(3)
    for d in range(planes):
        for from_core in (partner, partner + across - me):
            relay(lax.rem(from_core + n - 4 * d, n), partner, psend.at[d]).wait_recv()

    for copy in own:
        copy.wait_send()
    pass_on(chip, across, side_sem.at[chip]).wait_send()
    for d in range(planes):
        relay(me, partner, psend.at[4 + d]).wait_send()
        if d:
            line(d, me, across).wait_send()
            line_far(d, across).wait_send()
            transfer(d, me).wait_send()
            relay(me, partner, psend.at[d]).wait_send()
            for here, head in arrivals(d, chip):
                @pl.when(here)
                def _():
                    pass_on(head, across, side_sem.at[head]).wait_send()
        if d < planes - 1:
            for here, head, target, sem in along(d):
                @pl.when(here)
                def _():
                    pass_on(head, target, sem).wait_send()
    others_half = pl.ds(pl.multiple_of((1 - dp) * part_rows, 16), part_rows)
    for k in range(1, n // 2):
        head = lax.rem(chip + k, n // 2)
        swap(head).wait_send()
        pltpu.make_async_remote_copy(
            src_ref=w_out.at[head, :, others_half], dst_ref=w_out.at[head, :, others_half],
            send_sem=swap_sem.at[head], recv_sem=xrecv.at[head],
            device_id=(1 - dp, me), device_id_type=MESH).wait_recv()
    for copy in notes:
        copy.wait()


def lookup_exchange(n, rows, note, w):
    return pl.pallas_call(
        functools.partial(lookup_kernel, n),
        out_shape=[
            jax.ShapeDtypeStruct((n,) + rows.shape[1:], rows.dtype),
            jax.ShapeDtypeStruct((2, n) + note.shape, note.dtype),
            jax.ShapeDtypeStruct((n // 2,) + w.shape, w.dtype),
        ],
        in_specs=[vmem()] * 3,
        out_specs=[vmem()] * 3,
        scratch_shapes=[pltpu.VMEM((4,) + rows.shape[1:], rows.dtype)] + [pltpu.SemaphoreType.DMA((size,)) for size in (4, 4, 4, 8, n, 4, 2 * n, 2 * n, 4, 4, n // 2, n // 2, n // 2, n // 2)],
        compiler_params=pltpu.CompilerParams(collective_id=0, has_side_effects=True, vmem_limit_bytes=VMEM_LIMIT),
        cost_estimate=pl.CostEstimate(flops=50_000_000_000, bytes_accessed=8_000_000, transcendentals=0),
        name="lookup_exchange",
    )(rows, note, w)


def attend_kernel(n, heads, head_dim, got_ref, at_ref, pos_ref, gain_ref, beta_ref, w_ref, bias_ref, wo_ref,
                  out_ref, embed_ref, proj_ref, tok, w_all, qkv, ctx, acc, pos_seq, pos_own, psend_sem, precv_sem,
                  csend_sem, crecv_sem, osend_sem, orecv_sem, load_sem):
    me = lax.axis_index("tp")
    dp = lax.axis_index("dp")
    core = lax.rem(me, 2)
    chip = me // 2
    side = lax.rem(chip, 2)
    partner = me + 1 - 2 * core
    across = me + 2 - 4 * side
    total_rows, width = got_ref.shape
    half, block = pos_seq.shape[0], pos_own.shape[0]
    batch = embed_ref.shape[0]
    pad = LANES
    group = 4 * head_dim
    q_rows = 4 * block
    step = 256
    steps = half // step

    loads = [
        pltpu.make_async_copy(pos_ref.at[pl.ds(pl.multiple_of(core * half, 32), half)], pos_seq, load_sem.at[3 * heads]),
        pltpu.make_async_copy(pos_ref.at[pl.ds(pl.multiple_of(me * block, 32), block)], pos_own, load_sem.at[3 * heads + 1])]
    for head in range(heads):
        for part in range(3):
            start = 2 * heads * pad + head * head_dim if part == 2 else (part * heads + head) * pad
            loads.append(pltpu.make_async_copy(w_ref.at[head, part], w_all.at[pl.ds(start, head_dim)], load_sem.at[3 * head + part]))
    for load in loads:
        load.start()
    for h in range(2 * heads):
        w_all[pl.ds(h * pad + head_dim, pad - head_dim), :] = jnp.zeros((pad - head_dim, width), w_all.dtype)
    greet([(dp, lax.rem(me + k, n)) for k in range(1, n)])
    for load in loads[:2]:
        load.wait()

    def proj_at(source):
        return proj_ref.at[lax.rem(source, 2) * (n // 2) + source // 2]

    def spread(source, target, sem, first=False):
        return pltpu.make_async_remote_copy(
            src_ref=wo_ref if first else proj_at(source), dst_ref=proj_at(source),
            send_sem=osend_sem.at[sem], recv_sem=orecv_sem.at[source], device_id=(dp, target), device_id_type=MESH)

    for d in (2, 1, 3):
        spread(me, lax.rem(me + 4 * d, n), 4 * d, True).start()
    for i, target in enumerate((across, partner)):
        spread(me, target, 1 + i, True).start()
    proj_ref[core * (n // 2) + chip] = wo_ref[...]

    def table_rows(start, size):
        hit = at_ref[pl.ds(pl.multiple_of(start, 64), size), :] == lax.broadcasted_iota(jnp.int32, (size, total_rows), 1)
        return jnp.dot(hit.astype(jnp.bfloat16), got_ref[...], preferred_element_type=jnp.float32)

    def share(t):
        at = pl.ds(pl.multiple_of(core * half + t * step, step), step)
        return pltpu.make_async_remote_copy(
            src_ref=tok.at[at], dst_ref=tok.at[at], send_sem=psend_sem.at[t], recv_sem=precv_sem.at[t],
            device_id=(dp, partner), device_id_type=MESH)

    def embed_step(t, _):
        at = pl.ds(pl.multiple_of(t * step, step), step)
        rows = table_rows(t * step, step) + pos_seq[at, :].astype(jnp.float32)
        values = rows.astype(jnp.bfloat16).astype(jnp.float32)
        tok[pl.ds(pl.multiple_of(core * half + t * step, step), step), :] = layer_norm(values, gain_ref[...], beta_ref[...]).astype(tok.dtype)
        @pl.when(t > 0)
        def _():
            share(t - 1).start()
        return 0

    lax.fori_loop(0, steps, embed_step, 0)
    for load in loads[2:]:
        load.wait()

    def project(part, _):
        @pl.when(part == 1)
        def _():
            for t in range(steps):
                share(t).wait_recv()
        at_rows = pl.ds(pl.multiple_of(lax.rem(core + part, 2) * half, step), half)

        def columns(i, _):
            at = pl.ds(pl.multiple_of(i * 256, 256), 256)
            out = lax.dot_general(tok[at_rows, :], w_all[at, :], nt, preferred_element_type=jnp.float32)
            qkv[at_rows, at] = (out + bias_ref[:, at]).astype(qkv.dtype)
            @pl.when(jnp.logical_and(part == 0, i == 0))
            def _():
                share(steps - 1).start()
            return 0

        lax.fori_loop(0, w_all.shape[0] // 256, columns, 0)
        return 0

    scale = head_dim ** -0.5 * 1.4426950408889634
    lane_head = lax.broadcasted_iota(jnp.int32, (1, group), 1) // head_dim
    causal = lax.broadcasted_iota(jnp.int32, (q_rows, q_rows), 0) >= lax.broadcasted_iota(jnp.int32, (q_rows, q_rows), 1)
    nt = (((1,), (1,)), ((), ()))

    def delivery(p, source, g):
        lanes = pl.ds(pl.multiple_of(g * group, pad), group)
        return pltpu.make_async_remote_copy(
            src_ref=ctx.at[p, :, lanes], dst_ref=out_ref.at[source, :, lanes],
            send_sem=csend_sem.at[g * n + p], recv_sem=crecv_sem.at[g * n + source],
            device_id=(dp, p), device_id_type=MESH)

    lax.fori_loop(0, 2, project, 0)
    for d in range(1, 4):
        source = lax.rem(me + n - 4 * d, n)
        spread(source, across, 0).wait_recv()
        for i, target in enumerate((across, partner)):
            spread(source, target, 4 * d + 1 + i).start()

    for number, j in enumerate((2, 0, 3, 1)):
        keys = (j + 1) * q_rows
        done = j * q_rows

        def head_group(g, _):
            v_at = pl.ds(pl.multiple_of(2 * heads * pad + g * group, pad), group)

            def one_head(i):
                h = 4 * g + i
                q = qkv[done:keys, pl.ds(pl.multiple_of(h * pad, pad), pad)]
                k_at = pl.ds(pl.multiple_of((heads + h) * pad, pad), pad)
                near = lax.dot_general(q, qkv[done:keys, k_at], nt, preferred_element_type=jnp.float32)
                near = jnp.where(causal, near, -jnp.inf)
                top = jnp.max(near, axis=1, keepdims=True)
                if j:
                    far = lax.dot_general(q, qkv[0:done, k_at], nt, preferred_element_type=jnp.float32)
                    top = jnp.maximum(top, jnp.max(far, axis=1, keepdims=True))
                top = top * scale
                near = jnp.exp2(near * scale - top)
                total = jnp.sum(near, axis=1, keepdims=True)
                if j:
                    far = jnp.exp2(far * scale - top)
                    total = total + jnp.sum(far, axis=1, keepdims=True)
                part = 1.0 / total
                mine = lane_head == i
                v = jnp.where(mine, qkv[done:keys, v_at], jnp.zeros((), qkv.dtype))
                out = jnp.dot((near * part).astype(jnp.bfloat16), v, preferred_element_type=jnp.float32)
                if j:
                    v = jnp.where(mine, qkv[0:done, v_at], jnp.zeros((), qkv.dtype))
                    out = out + jnp.dot((far * part).astype(jnp.bfloat16), v, preferred_element_type=jnp.float32)
                acc[...] += out

            def two_heads(i, _):
                one_head(2 * i)
                one_head(2 * i + 1)
                return 0

            acc[...] = jnp.zeros_like(acc)
            lax.fori_loop(0, 2, two_heads, 0)
            for r in range(4):
                ctx[4 * j + r, :, pl.ds(pl.multiple_of(g * group, pad), group)] = acc[r * block:(r + 1) * block, :].astype(ctx.dtype)
            for r in range(4):
                p = 4 * j + r
                @pl.when(me != p)
                def _():
                    delivery(p, me, g).start()
            return 0

        lax.fori_loop(0, heads // 4, head_group, 0)
        if number == 1:
            for d in range(4):
                source = lax.rem(across + n - 4 * d, n)
                spread(source, across, 0).wait_recv()
                spread(source, partner, 4 * d + 3).start()

    out_ref[me] = ctx[me]
    pos_pair = jnp.concatenate([pos_own[...].astype(jnp.float32)] * 2, axis=0)

    def own_step(t, _):
        rows = table_rows(half + t * 2 * block, 2 * block) + pos_pair
        embed_ref[pl.ds(2 * t, 2)] = rows.astype(embed_ref.dtype).reshape(2, block, width)
        return 0

    lax.fori_loop(0, batch // 2, own_step, 0)
    for d in range(4):
        for from_core in (partner, partner + across - me):
            spread(lax.rem(from_core + n - 4 * d, n), partner, 0).wait_recv()
    for sem in [1, 2, 3] + [4 * d + i for d in (1, 2, 3) for i in range(4)]:
        spread(me, partner, sem).wait_send()
    for k in range(1, n):
        peer = lax.rem(me + k, n)
        for g in range(heads // 4):
            delivery(peer, me, g).wait_send()
            delivery(me, peer, g).wait_recv()
    for t in range(steps):
        share(t).wait_send()


def attend_exchange(n, batch, got, at, pos, gain, beta, w, bias, wo):
    heads, _, head_dim, width = w.shape
    seq_len = pos.shape[0]
    block, inner, columns = seq_len // n, heads * head_dim, bias.shape[1]
    steps = seq_len // 2 // 256
    hbm = pl.BlockSpec(memory_space=pl.ANY)
    return pl.pallas_call(
        functools.partial(attend_kernel, n, heads, head_dim),
        out_shape=[
            jax.ShapeDtypeStruct((n, block, inner), got.dtype),
            jax.ShapeDtypeStruct((batch, block, width), got.dtype),
            jax.ShapeDtypeStruct((n,) + wo.shape, wo.dtype),
        ],
        in_specs=[vmem(), vmem(), hbm, vmem(), vmem(), hbm, vmem(), vmem()],
        out_specs=[vmem()] * 3,
        scratch_shapes=[
            pltpu.VMEM((seq_len, width), got.dtype),
            pltpu.VMEM((columns, width), got.dtype),
            pltpu.VMEM((seq_len, columns), got.dtype),
            pltpu.VMEM((n, block, inner), got.dtype),
            pltpu.VMEM((4 * block, 4 * head_dim), jnp.float32),
            pltpu.VMEM((seq_len // 2, width), got.dtype),
            pltpu.VMEM((block, width), got.dtype),
        ] + [pltpu.SemaphoreType.DMA((size,)) for size in (steps, steps, 2 * n, 2 * n, n, n, 3 * heads + 2)],
        compiler_params=pltpu.CompilerParams(collective_id=1, has_side_effects=True, vmem_limit_bytes=VMEM_LIMIT),
        cost_estimate=pl.CostEstimate(flops=50_000_000_000, bytes_accessed=20_000_000, transcendentals=0),
        name="attend_exchange",
    )(got, at, pos, gain, beta, w, bias, wo)


def solution(mesh):
    n = mesh.shape["tp"]

    def local_step(token_ids, word_shard, pos_table, ln_gain, ln_bias, w_qkv, b_qkv, w_out, b_out):
        shard_rows, model_dim = word_shard.shape
        batch, seq_len = token_ids.shape
        head_dim = w_qkv.shape[-1]
        block_len = seq_len // n
        tokens = batch * block_len
        me = lax.axis_index("tp")
        chips = n // 2
        chip_ids = jnp.concatenate([
            token_ids.reshape(batch, chips, 2 * block_len).transpose(1, 0, 2).reshape(chips, -1),
            token_ids], axis=1)
        hi_rows = shard_rows // LANES
        lanes = jnp.arange(LANES)

        def one_hot(hit):
            return hit.astype(jnp.bfloat16)

        def listing(present):
            present = one_hot(present > 0.5)
            in_row = jnp.einsum("...hl,lm->...hm", present, one_hot(lanes[:, None] <= lanes), preferred_element_type=jnp.float32)
            rows = jnp.arange(hi_rows)
            before = jnp.einsum("gh,...h->...g", one_hot(rows[:, None] > rows), in_row[..., -1].astype(jnp.bfloat16), preferred_element_type=jnp.float32)
            return in_row + before[..., None], present.astype(jnp.float32)

        low = one_hot((chip_ids % LANES)[:, :, None] == lanes)
        high = one_hot((chip_ids // LANES - me * hi_rows)[:, None, :] == jnp.arange(hi_rows)[:, None])
        present = jnp.einsum("zht,ztl->zhl", high, low, preferred_element_type=jnp.float32)
        counted, _ = listing(present)
        counted = counted.reshape(chips, shard_rows)

        def rows_to_send(first):
            target = (first + jnp.arange(SLOTS)).astype(jnp.float32)
            send_list = jnp.sum((counted[:, None, :] <= target[:, None]).astype(jnp.int32), axis=2)
            return jnp.take(word_shard, send_list.reshape(-1), axis=0, mode="clip").reshape(chips, SLOTS, model_dim)

        my_ids = lax.dynamic_index_in_dim(chip_ids, me // 2, 0, keepdims=False)
        high = one_hot((my_ids // LANES)[None, :] == jnp.arange(n * hi_rows)[:, None])
        low = one_hot((my_ids % LANES)[:, None] == lanes)
        present = jnp.dot(high, low, preferred_element_type=jnp.float32)
        my_counted, my_present = listing(present.reshape(n, hi_rows, LANES))
        slots = (my_counted - my_present).reshape(n * hi_rows, LANES).astype(jnp.int32)
        parts = jnp.concatenate([slots // 64, slots % 64], axis=1).astype(jnp.bfloat16)
        seq_ids = lax.dynamic_slice(token_ids, (me // 2, lax.rem(me, 2) * tokens), (1, tokens))
        own_ids = lax.dynamic_slice_in_dim(token_ids, me * block_len, block_len, axis=1)
        wanted = jnp.concatenate([seq_ids.reshape(-1), own_ids.reshape(-1)])
        found = jnp.dot(one_hot((wanted // LANES)[:, None] == jnp.arange(n * hi_rows)), parts, preferred_element_type=jnp.float32)
        found = jnp.sum(jnp.where(((wanted % LANES)[:, None] == lanes)[:, None, :], found.reshape(-1, 2, LANES), 0.0), axis=2).astype(jnp.int32)
        slot = found[:, 0] * 64 + found[:, 1]
        owner = wanted // shard_rows

        note = jnp.pad(b_qkv[:, 0, :], ((0, 5), (0, LANES - head_dim)))
        note = note.at[3].set(jnp.max(counted))
        w_own = w_qkv[:, :, 0, :].transpose(1, 2, 0)
        got_rows, notes, w_heads = lookup_exchange(n, rows_to_send(0), note, w_own)
        got_rows = got_rows.reshape(n * SLOTS, model_dim)
        all_count = jnp.max(notes[:, :, 3, 0]).astype(jnp.int32)

        def fetch_all(carry):
            def next_round(inner):
                first, rows = inner
                send = jnp.broadcast_to(rows_to_send(first)[:, None], (chips, 2, SLOTS, model_dim)).reshape(n, SLOTS, model_dim)
                got = lax.all_to_all(send, "tp", 0, 0, tiled=True).reshape(n * SLOTS, model_dim)
                picked = jnp.take(got, owner * SLOTS + jnp.clip(slot - first, 0, SLOTS - 1), axis=0, mode="clip")
                return first + SLOTS, jnp.where((slot >= first)[:, None], picked, rows)

            _, rows = lax.while_loop(lambda inner: inner[0] < all_count, next_round, (jnp.int32(0), jnp.zeros((2 * tokens, model_dim), jnp.bfloat16)))
            return jnp.int32(0), jnp.pad(rows, ((0, n * SLOTS - 2 * tokens), (0, 0))), jnp.arange(2 * tokens)

        _, got_rows, row_of = lax.while_loop(lambda carry: carry[0] > SLOTS, fetch_all, (all_count, got_rows, owner * SLOTS + slot))

        b_heads = lax.dynamic_index_in_dim(notes[0, :, :3, :head_dim].reshape(n // 2, 2, 3, head_dim), lax.rem(me, 2), 1, keepdims=False)
        bias_qk = jnp.pad(b_heads[:, :2], ((0, 0), (0, 0), (0, LANES - head_dim))).transpose(1, 0, 2).reshape(1, -1)
        bias = jnp.concatenate([bias_qk, b_heads[:, 2].reshape(1, -1)], axis=1)
        got_context, embed, w_proj = attend_exchange(n, batch, got_rows, row_of[:, None], pos_table, ln_gain[None], ln_bias[None], w_heads, bias, w_out[0])
        got_context = got_context.reshape(batch, 2, block_len, n // 2 * head_dim)
        out_block = jnp.einsum("qcsf,cfd->qsd", got_context, w_proj.reshape(2, n // 2 * head_dim, model_dim), preferred_element_type=jnp.float32)
        resid_out = (embed.astype(jnp.float32) + out_block + b_out).astype(jnp.bfloat16)
        return resid_out, embed

    in_specs = (P("dp", None), P("tp", None), P(None, None), P(None), P(None), P(None, None, "tp", None), P(None, "tp", None), P("tp", None, None), P(None))
    out_specs = (P("dp", "tp", None), P("dp", "tp", None))
    return jax.shard_map(local_step, mesh=mesh, in_specs=in_specs, out_specs=out_specs, check_vma=False)
```
